8 devices in a mesh: dp: 2 (over z, y), sp: 4 (over x, core).
Axes of the slice: x: 2, y: 2, z: 1, core: 2. Of those that a mesh axis runs over, the one named last changes fastest.
Arguments:
- signal: bfloat16 [4, 1024, 512], P('dp', 'sp'), parts along dimension 0
- cond_feats: bfloat16 [4, 1024, 256], P('dp', 'sp'), parts along dimension 0
- w_now: bfloat16 [10, 512, 1024], replicated
- w_past: bfloat16 [10, 512, 1024], replicated
- w_cond: bfloat16 [10, 256, 1024], replicated
- b_gate: float32 [10, 1024], replicated
- w_res: bfloat16 [10, 512, 512], replicated
- w_skip: bfloat16 [10, 512, 256], replicated
Outputs:
- output 1: float32 [4, 1024, 512], P('dp', 'sp'), parts along dimension 0
- output 2: float32 [4, 1024, 256], P('dp', 'sp'), parts along dimension 0
There are 2 independent parts. The reference program is written for one: setup_inputs(seed, part) draws one part's arguments, and reference() takes and returns one part's arrays. A program takes and returns all parts, laid end to end along the dimension named above; an argument that names none is the same for every part.
All inputs are finite; a program needn't handle non-finite values.
Results may differ from the reference program's by a relative error of at most 0.00641958.
Values are sent between devices in bfloat16 or wider.
A program may use at most 1 GiB of HBM per device.

```python
import jax
import jax.numpy as jnp

BATCH = 2
SEQ_LEN = 1024
CHANNELS = 512
SKIP_CH = 256
COND_CH = 256
LAYERS = 10


def setup_inputs(seed: int = 0, part: int = 0) -> dict:
    part_key = jax.random.fold_in(jax.random.key(seed), part)
    sig_key, cond_key = jax.random.split(part_key, 2)
    weight_keys = jax.random.split(jax.random.key(seed + 1), 6)
    gate_scale = (2 * CHANNELS + COND_CH) ** -0.5
    out_scale = CHANNELS ** -0.5
    signal = jax.random.normal(sig_key, (BATCH, SEQ_LEN, CHANNELS), jnp.float32)
    cond_feats = jax.random.normal(cond_key, (BATCH, SEQ_LEN, COND_CH), jnp.float32)
    w_now = jax.random.normal(weight_keys[0], (LAYERS, CHANNELS, 2 * CHANNELS), jnp.float32) * gate_scale
    w_past = jax.random.normal(weight_keys[1], (LAYERS, CHANNELS, 2 * CHANNELS), jnp.float32) * gate_scale
    w_cond = jax.random.normal(weight_keys[2], (LAYERS, COND_CH, 2 * CHANNELS), jnp.float32) * gate_scale
    b_gate = 0.5 * jax.random.normal(weight_keys[3], (LAYERS, 2 * CHANNELS), jnp.float32)
    w_res = jax.random.normal(weight_keys[4], (LAYERS, CHANNELS, CHANNELS), jnp.float32) * out_scale
    w_skip = jax.random.normal(weight_keys[5], (LAYERS, CHANNELS, SKIP_CH), jnp.float32) * out_scale
    return {
        'signal': signal.astype(jnp.bfloat16),
        'cond_feats': cond_feats.astype(jnp.bfloat16),
        'w_now': w_now.astype(jnp.bfloat16),
        'w_past': w_past.astype(jnp.bfloat16),
        'w_cond': w_cond.astype(jnp.bfloat16),
        'b_gate': b_gate,
        'w_res': w_res.astype(jnp.bfloat16),
        'w_skip': w_skip.astype(jnp.bfloat16),
    }


def reference(signal, cond_feats, w_now, w_past, w_cond, b_gate, w_res, w_skip):
    resid = signal.astype(jnp.float32)
    skip_sum = jnp.zeros((BATCH, SEQ_LEN, SKIP_CH), jnp.float32)
    cond_wide = cond_feats.astype(jnp.float32)
    for layer in range(LAYERS):
        dilation = 2 ** layer
        now_in = resid.astype(jnp.bfloat16)
        past_in = jnp.concatenate([jnp.zeros((BATCH, dilation, CHANNELS), jnp.bfloat16), now_in[:, :SEQ_LEN - dilation]], axis=1)
        gate_pre = (jnp.einsum('bsc,cg->bsg', now_in.astype(jnp.float32), w_now[layer].astype(jnp.float32))
                    + jnp.einsum('bsc,cg->bsg', past_in.astype(jnp.float32), w_past[layer].astype(jnp.float32))
                    + jnp.einsum('bsc,cg->bsg', cond_wide, w_cond[layer].astype(jnp.float32))
                    + b_gate[layer])
        gated = (jnp.tanh(gate_pre[..., :CHANNELS]) * jax.nn.sigmoid(gate_pre[..., CHANNELS:])).astype(jnp.bfloat16)
        gated_wide = gated.astype(jnp.float32)
        resid = resid + jnp.einsum('bsc,cd->bsd', gated_wide, w_res[layer].astype(jnp.float32))
        skip_sum = skip_sum + jnp.einsum('bsc,cd->bsd', gated_wide, w_skip[layer].astype(jnp.float32))
    return resid, skip_sum
```

```python
import functools

import jax
import jax.numpy as jnp
from jax import lax
from jax.experimental import pallas as pl
from jax.experimental.pallas import tpu as pltpu
from jax.sharding import PartitionSpec as P

BF16, F32 = jnp.bfloat16, jnp.float32
MESH = pl.DeviceIdType.MESH
AHEAD = 3


def stack_kernel(n_sp, signal, cond, w_now, w_past, w_cond, b_gate, w_res, w_skip, h_out, skip_out,
                 u, c, bias, w_in, w_mix, h, skip,
                 sig_sem, cond_sem, bias_sem, w_sem, send_sem, recv_sem, out_sem):
    batch, layers, two_span, ch = u.shape
    span = two_span // 2
    cond_ch = c.shape[2]
    dp, me = lax.axis_index('dp'), lax.axis_index('sp')

    def weight_copies(layer):
        pairs = (
            (w_now.at[layer], w_in.at[layer, pl.ds(0, ch)]),
            (w_cond.at[layer], w_in.at[layer, pl.ds(ch, cond_ch)]),
            (w_past.at[layer], w_in.at[layer, pl.ds(ch + cond_ch, ch)]),
            (w_res.at[layer], w_mix.at[layer, :, pl.ds(0, ch)]),
            (w_skip.at[layer], w_mix.at[layer, :, pl.ds(ch, skip.shape[2])]),
        )
        return [pltpu.make_async_copy(src, dst, w_sem.at[layer, i]) for i, (src, dst) in enumerate(pairs)]

    def hops(layer):
        return max(1, 2 ** layer // span)

    def halo(layer):
        return min(max(16, 2 ** layer), span)

    def edge_copy(s, layer):
        rows = halo(layer)
        return pltpu.make_async_remote_copy(
            src_ref=u.at[s, layer, pl.ds(2 * span - rows, rows)],
            dst_ref=u.at[s, layer, pl.ds(span - rows, rows)],
            send_sem=send_sem.at[s, layer], recv_sem=recv_sem.at[s, layer],
            device_id=(dp, lax.rem(me + hops(layer), n_sp)), device_id_type=MESH)

    def send_edge(s, layer):
        @pl.when(me + hops(layer) < n_sp)
        def _():
            edge_copy(s, layer).start()

    sig_in = [pltpu.make_async_copy(signal.at[s], u.at[s, 0, pl.ds(span, span)], sig_sem.at[s]) for s in range(batch)]
    cond_in = [pltpu.make_async_copy(cond.at[s], c.at[s], cond_sem.at[s]) for s in range(batch)]
    bias_in = pltpu.make_async_copy(b_gate, bias, bias_sem)
    sig_in[0].start()
    cond_in[0].start()
    bias_in.start()
    for layer in range(AHEAD):
        for copy in weight_copies(layer):
            copy.start()
    for s in range(1, batch):
        sig_in[s].start()
        cond_in[s].start()

    barrier = pltpu.get_barrier_semaphore()
    for off in range(1, n_sp):
        pl.semaphore_signal(barrier, inc=1, device_id=(dp, lax.rem(me + off, n_sp)), device_id_type=MESH)

    for layer in range(layers):
        @pl.when(me < hops(layer))
        def _():
            rows = halo(layer)
            for s in range(batch):
                u[s, layer, span - rows:span] = jnp.zeros((rows, ch), BF16)

    pl.semaphore_wait(barrier, n_sp - 1)

    for s in range(batch):
        sig_in[s].wait()
        send_edge(s, 0)
    for s in range(batch):
        cond_in[s].wait()
    bias_in.wait()

    def step(s, layer):
        dilation = 2 ** layer

        @pl.when(s == 0)
        def _():
            if layer + AHEAD < layers:
                for copy in weight_copies(layer + AHEAD):
                    copy.start()
            for copy in weight_copies(layer):
                copy.wait()

        @pl.when(me >= hops(layer))
        def _():
            edge_copy(s, layer).wait_recv()

        now = u[s, layer, span:]
        if dilation < 16:
            wide = u[s, layer, span - 16:].astype(F32)
            past = pltpu.roll(wide, dilation, axis=0)[16:].astype(BF16)
        else:
            past = u[s, layer, span - halo(layer):2 * span - halo(layer)]
        x = jnp.concatenate([now, c[s], past], axis=1)
        half = ch // 2
        gated = []
        for i in range(2):
            lo, hi = i * half, (i + 1) * half
            zf = jnp.dot(x, w_in[layer, :, lo:hi], preferred_element_type=F32) + bias[layer:layer + 1, lo:hi]
            zg = jnp.dot(x, w_in[layer, :, ch + lo:ch + hi], preferred_element_type=F32) + bias[layer:layer + 1, ch + lo:ch + hi]
            gated.append((jnp.tanh(zf) * (0.5 * jnp.tanh(0.5 * zg) + 0.5)).astype(BF16))
        a = jnp.concatenate(gated, axis=1)
        base = now.astype(F32) if layer == 0 else h[s]
        new_h = base + jnp.dot(a, w_mix[layer, :, :ch], preferred_element_type=F32)
        h[s] = new_h
        if layer + 1 < layers:
            u[s, layer + 1, span:] = new_h.astype(BF16)
        new_skip = jnp.dot(a, w_mix[layer, :, ch:], preferred_element_type=F32)
        skip[s] = new_skip if layer == 0 else skip[s] + new_skip
        if layer + 1 < layers:
            send_edge(s, layer + 1)
        else:
            pltpu.make_async_copy(h.at[s], h_out.at[s], out_sem.at[s, 0]).start()
            pltpu.make_async_copy(skip.at[s], skip_out.at[s], out_sem.at[s, 1]).start()

    def run(i, carry):
        early = jnp.where(i < 9, i, jnp.where(i < 18, i + 1, jnp.where(i < 19, 9, 19)))
        late = jnp.where(i < 8, i, jnp.where(i < 10, i + 2, jnp.where(i < 11, 8, jnp.where(
            i < 17, i + 1, jnp.where(i < 18, 9, i)))))
        code = jnp.where(me < n_sp // 2, early, late)
        s, which = code // layers, code % layers
        for layer in range(layers):
            @pl.when(which == layer)
            def _():
                step(s, layer)
        return carry

    lax.fori_loop(0, batch * layers, run, 0)

    for s in range(batch):
        pltpu.make_async_copy(h.at[s], h_out.at[s], out_sem.at[s, 0]).wait()
        pltpu.make_async_copy(skip.at[s], skip_out.at[s], out_sem.at[s, 1]).wait()
        for layer in range(layers):
            @pl.when(me + hops(layer) < n_sp)
            def _():
                edge_copy(s, layer).wait_send()


def solution(mesh):
    n_sp = mesh.shape['sp']

    def local_stack(signal, cond_feats, w_now, w_past, w_cond, b_gate, w_res, w_skip):
        batch, span, ch = signal.shape
        layers, cond_ch, skip_ch = w_now.shape[0], cond_feats.shape[2], w_skip.shape[2]
        anywhere = pl.BlockSpec(memory_space=pl.ANY)
        return pl.pallas_call(
            functools.partial(stack_kernel, n_sp),
            out_shape=[jax.ShapeDtypeStruct((batch, span, ch), F32), jax.ShapeDtypeStruct((batch, span, skip_ch), F32)],
            in_specs=[anywhere] * 8,
            out_specs=[anywhere] * 2,
            scratch_shapes=[
                pltpu.VMEM((batch, layers, 2 * span, ch), BF16),
                pltpu.VMEM((batch, span, cond_ch), BF16),
                pltpu.VMEM((layers, 2 * ch), F32),
                pltpu.VMEM((layers, 2 * ch + cond_ch, 2 * ch), BF16),
                pltpu.VMEM((layers, ch, ch + skip_ch), BF16),
                pltpu.VMEM((batch, span, ch), F32),
                pltpu.VMEM((batch, span, skip_ch), F32),
                pltpu.SemaphoreType.DMA((batch,)),
                pltpu.SemaphoreType.DMA((batch,)),
                pltpu.SemaphoreType.DMA,
                pltpu.SemaphoreType.DMA((layers, 5)),
                pltpu.SemaphoreType.DMA((batch, layers)),
                pltpu.SemaphoreType.DMA((batch, layers)),
                pltpu.SemaphoreType.DMA((batch, 2)),
            ],
            compiler_params=pltpu.CompilerParams(collective_id=0, has_side_effects=True, vmem_limit_bytes=60 * 2 ** 20),
        )(signal, cond_feats, w_now, w_past, w_cond, b_gate, w_res, w_skip)

    seq_spec = P('dp', 'sp', None)
    return jax.shard_map(local_stack, mesh=mesh,
                         in_specs=(seq_spec, seq_spec, P(), P(), P(), P(), P(), P()),
                         out_specs=(seq_spec, seq_spec), check_vma=False)
```

```python
import functools

import jax
import jax.numpy as jnp
from jax import lax
from jax.experimental import pallas as pl
from jax.experimental.pallas import tpu as pltpu
from jax.sharding import PartitionSpec as P

BF16, F32 = jnp.bfloat16, jnp.float32
MESH = pl.DeviceIdType.MESH
AHEAD = 2
PIECES = 8


def at_step(i, order):
    code = i + (order[-1] - (len(order) - 1))
    for j in range(len(order) - 2, -1, -1):
        if order[j] - j != order[j + 1] - (j + 1):
            code = jnp.where(i <= j, i + (order[j] - j), code)
    return code


def stack_kernel(n_sp, signal, cond, w_now, w_past, w_cond, b_gate, w_res, w_skip, h, skip,
                 u, acts, c, bias, w_in, w_mix, w_sum,
                 sig_sem, cond_sem, bias_sem, w_sem, send_sem, recv_sem, far_send_sem, far_recv_sem):
    batch, layers, two_span, ch = u.shape
    span = two_span // 2
    cond_ch = c.shape[2]
    dp, me = lax.axis_index('dp'), lax.axis_index('sp')

    def weight_copies(layer):
        pairs = (
            (w_now.at[layer], w_in.at[layer, pl.ds(0, ch)]),
            (w_cond.at[layer], w_in.at[layer, pl.ds(ch, cond_ch)]),
            (w_past.at[layer], w_in.at[layer, pl.ds(ch + cond_ch, ch)]),
            (w_res.at[layer], w_mix.at[layer]),
            (w_skip.at[layer], w_sum.at[pl.ds(layer * ch, ch)]),
        )
        return [pltpu.make_async_copy(src, dst, w_sem.at[layer, i]) for i, (src, dst) in enumerate(pairs)]

    def hops(layer):
        return max(1, 2 ** layer // span)

    def halo(layer):
        return min(max(16, 2 ** layer), span)

    def edge_copy(s, layer):
        rows = halo(layer)
        return pltpu.make_async_remote_copy(
            src_ref=u.at[s, layer, pl.ds(2 * span - rows, rows)],
            dst_ref=u.at[s, layer, pl.ds(span - rows, rows)],
            send_sem=send_sem.at[s, layer], recv_sem=recv_sem.at[s, layer],
            device_id=(dp, lax.rem(me + hops(layer), n_sp)), device_id_type=MESH)

    def send_edge(s, layer):
        @pl.when(me + hops(layer) < n_sp)
        def _():
            edge_copy(s, layer).start()

    def far_copy(s, piece):
        rows = span // PIECES
        return pltpu.make_async_remote_copy(
            src_ref=u.at[s, layers - 1, pl.ds(span + piece * rows, rows)],
            dst_ref=u.at[s, layers - 1, pl.ds(piece * rows, rows)],
            send_sem=far_send_sem.at[s, piece], recv_sem=far_recv_sem.at[s, piece],
            device_id=(dp, lax.rem(me + hops(layers - 1), n_sp)), device_id_type=MESH)

    sig_in = [pltpu.make_async_copy(signal.at[s], u.at[s, 0, pl.ds(span, span)], sig_sem.at[s]) for s in range(batch)]
    cond_in = [pltpu.make_async_copy(cond.at[s], c.at[s], cond_sem.at[s]) for s in range(batch)]
    bias_in = pltpu.make_async_copy(b_gate, bias, bias_sem)
    sig_in[0].start()
    cond_in[0].start()
    bias_in.start()
    for layer in range(AHEAD):
        for copy in weight_copies(layer):
            copy.start()
    for s in range(1, batch):
        sig_in[s].start()
        cond_in[s].start()

    barrier = pltpu.get_barrier_semaphore()
    for off in range(1, n_sp):
        pl.semaphore_signal(barrier, inc=1, device_id=(dp, lax.rem(me + off, n_sp)), device_id_type=MESH)

    for layer in range(layers):
        @pl.when(me < hops(layer))
        def _():
            rows = halo(layer)
            for s in range(batch):
                u[s, layer, span - rows:span] = jnp.zeros((rows, ch), BF16)

    pl.semaphore_wait(barrier, n_sp - 1)

    for s in range(batch):
        sig_in[s].wait()
        send_edge(s, 0)
    for s in range(batch):
        cond_in[s].wait()
    bias_in.wait()

    def step(s, layer):
        dilation = 2 ** layer

        @pl.when(s == 0)
        def _():
            if layer + AHEAD < layers:
                for copy in weight_copies(layer + AHEAD):
                    copy.start()
            for copy in weight_copies(layer):
                copy.wait()

        @pl.when(me >= hops(layer))
        def _():
            if layer == layers - 1:
                for piece in range(PIECES):
                    far_copy(s, piece).wait_recv()
            else:
                edge_copy(s, layer).wait_recv()

        now = u[s, layer, span:]
        if dilation < 16:
            wide = u[s, layer, span - 16:].astype(F32)
            past = pltpu.roll(wide, dilation, axis=0)[16:].astype(BF16)
        else:
            past = u[s, layer, span - halo(layer):2 * span - halo(layer)]
        x = jnp.concatenate([now, c[s], past], axis=1)
        half = ch // 2
        gated = []
        for i in range(2):
            lo, hi = i * half, (i + 1) * half
            zf = jnp.dot(x, w_in[layer, :, lo:hi], preferred_element_type=F32) + bias[layer:layer + 1, lo:hi]
            zg = jnp.dot(x, w_in[layer, :, ch + lo:ch + hi], preferred_element_type=F32) + bias[layer:layer + 1, ch + lo:ch + hi]
            gated.append((jnp.tanh(zf) * (0.5 * jnp.tanh(0.5 * zg) + 0.5)).astype(BF16))
        a = jnp.concatenate(gated, axis=1)
        base = now.astype(F32) if layer == 0 else h[s]
        new_h = base + jnp.dot(a, w_mix[layer], preferred_element_type=F32)
        h[s] = new_h
        if layer + 1 < layers:
            u[s, layer + 1, span:] = new_h.astype(BF16)
            acts[s, :, layer * ch:(layer + 1) * ch] = a
        else:
            skip[s] += jnp.dot(a, w_sum[layer * ch:], preferred_element_type=F32)
        if layer + 2 < layers:
            send_edge(s, layer + 1)

            @pl.when((s == 1) & (me + hops(layers - 1) < n_sp))
            def _():
                far_copy(0, layer).start()
        elif layer + 1 < layers:
            @pl.when((s == 1) & (me + hops(layers - 1) < n_sp))
            def _():
                for piece in range(PIECES):
                    far_copy(1, piece).start()

    def sum_skip(s):
        skip[s] = jnp.dot(acts[s], w_sum[:(layers - 1) * ch], preferred_element_type=F32)

    lead = [2 * k for k in range(9)]
    early = lead + [2 * k + 1 for k in range(9)] + [20, 21, 18, 19]
    late = lead[:8] + [1, 16] + [2 * k + 1 for k in range(1, 8)] + [20, 18, 17, 21, 19]

    def run(i, carry):
        code = jnp.where(me < n_sp // 2, at_step(i, early), at_step(i, late))
        s, which = code % batch, code // batch
        for layer in range(layers):
            @pl.when(which == layer)
            def _():
                step(s, layer)

        @pl.when(which == layers)
        def _():
            sum_skip(s)
        return carry

    lax.fori_loop(0, len(early), run, 0)

    for s in range(batch):
        for layer in range(layers - 1):
            @pl.when(me + hops(layer) < n_sp)
            def _():
                edge_copy(s, layer).wait_send()

        @pl.when(me + hops(layers - 1) < n_sp)
        def _():
            for piece in range(PIECES):
                far_copy(s, piece).wait_send()


def store_kernel(h, skip, h_out, skip_out, sem):
    copies = [pltpu.make_async_copy(h, h_out, sem.at[0]), pltpu.make_async_copy(skip, skip_out, sem.at[1])]
    for copy in copies:
        copy.start()
    for copy in copies:
        copy.wait()


def solution(mesh):
    n_sp = mesh.shape['sp']

    def local_stack(signal, cond_feats, w_now, w_past, w_cond, b_gate, w_res, w_skip):
        batch, span, ch = signal.shape
        layers, cond_ch, skip_ch = w_now.shape[0], cond_feats.shape[2], w_skip.shape[2]
        anywhere = pl.BlockSpec(memory_space=pl.ANY)
        in_vmem = pl.BlockSpec(memory_space=pltpu.VMEM)
        h, skip = pl.pallas_call(
            functools.partial(stack_kernel, n_sp),
            out_shape=[pltpu.VMEM((batch, span, ch), F32), pltpu.VMEM((batch, span, skip_ch), F32)],
            in_specs=[pl.BlockSpec(memory_space=pltpu.HBM)] * 8,
            out_specs=[in_vmem] * 2,
            scratch_shapes=[
                pltpu.VMEM((batch, layers, 2 * span, ch), BF16),
                pltpu.VMEM((batch, span, (layers - 1) * ch), BF16),
                pltpu.VMEM((batch, span, cond_ch), BF16),
                pltpu.VMEM((layers, 2 * ch), F32),
                pltpu.VMEM((layers, 2 * ch + cond_ch, 2 * ch), BF16),
                pltpu.VMEM((layers, ch, ch), BF16),
                pltpu.VMEM((layers * ch, skip_ch), BF16),
                pltpu.SemaphoreType.DMA((batch,)),
                pltpu.SemaphoreType.DMA((batch,)),
                pltpu.SemaphoreType.DMA,
                pltpu.SemaphoreType.DMA((layers, 5)),
                pltpu.SemaphoreType.DMA((batch, layers - 1)),
                pltpu.SemaphoreType.DMA((batch, layers - 1)),
                pltpu.SemaphoreType.DMA((batch, PIECES)),
                pltpu.SemaphoreType.DMA((batch, PIECES)),
            ],
            compiler_params=pltpu.CompilerParams(collective_id=0, has_side_effects=True, vmem_limit_bytes=60 * 2 ** 20),
        )(signal, cond_feats, w_now, w_past, w_cond, b_gate, w_res, w_skip)
        return pl.pallas_call(
            store_kernel,
            out_shape=[jax.ShapeDtypeStruct((batch, span, ch), F32), jax.ShapeDtypeStruct((batch, span, skip_ch), F32)],
            in_specs=[in_vmem] * 2,
            out_specs=[anywhere] * 2,
            scratch_shapes=[pltpu.SemaphoreType.DMA((2,))],
            compiler_params=pltpu.CompilerParams(vmem_limit_bytes=2 ** 20),
        )(h, skip)

    seq_spec = P('dp', 'sp', None)
    return jax.shard_map(local_stack, mesh=mesh,
                         in_specs=(seq_spec, seq_spec, P(), P(), P(), P(), P(), P()),
                         out_specs=(seq_spec, seq_spec), check_vma=False)
```

```python
import functools

import jax
import jax.numpy as jnp
from jax import lax
from jax.experimental import pallas as pl
from jax.experimental.pallas import tpu as pltpu
from jax.sharding import PartitionSpec as P

BF16, F32 = jnp.bfloat16, jnp.float32
MESH = pl.DeviceIdType.MESH
TILE = 16
AHEAD = 2
PIECES = 8


def at_step(i, order):
    code = 2 * i + (order[-1] - 2 * (len(order) - 1))
    for j in range(len(order) - 2, -1, -1):
        if order[j] - 2 * j != order[j + 1] - 2 * (j + 1):
            code = jnp.where(i <= j, 2 * i + (order[j] - 2 * j), code)
    return code


def stack_kernel(n_sp, signal, cond, w_now, w_past, w_cond, b_gate, w_res, w_skip, h, skip,
                 u, acts, z_part, c, bias, w_in, w_mix, w_sum,
                 sig_sem, cond_sem, bias_sem, w_sem, sum_sem, send_sem, recv_sem, far_send_sem, far_recv_sem):
    batch, layers, span, ch = u.shape[0], w_in.shape[0], h.shape[1], h.shape[2]
    last, cond_ch = layers - 1, c.shape[2]
    dp, me = lax.axis_index('dp'), lax.axis_index('sp')

    sizes = [min(max(TILE, 2 ** k), span) for k in range(last)]
    groups = [(sizes.index(rows), len(sizes) - sizes[::-1].index(rows), rows) for rows in sorted(set(sizes))]
    far_hops = 2 ** last // span

    def start_weights(layer):
        slot = lax.rem(layer, AHEAD + 1)
        for src, dst in ((w_now.at[layer], w_in.at[layer, pl.ds(0, ch)]),
                         (w_cond.at[layer], w_in.at[layer, pl.ds(ch, cond_ch)]),
                         (w_past.at[layer], w_in.at[layer, pl.ds(ch + cond_ch, ch)])):
            pltpu.make_async_copy(src, dst, w_sem.at[slot, 0]).start()
        pltpu.make_async_copy(w_res.at[layer], w_mix.at[layer], w_sem.at[slot, 1]).start()

    def landed(ref, sem):
        pltpu.make_async_copy(ref, ref, sem).wait()

    def await_weights(layer):
        slot = lax.rem(layer, AHEAD + 1)
        landed(w_in.at[layer], w_sem.at[slot, 0])
        landed(w_mix.at[layer], w_sem.at[slot, 1])

    def edge_copy(s, layer, rows):
        return pltpu.make_async_remote_copy(
            src_ref=u.at[s, layer, pl.ds(2 * span - rows, rows)],
            dst_ref=u.at[s, layer, pl.ds(span - rows, rows)],
            send_sem=send_sem.at[s], recv_sem=recv_sem.at[s, layer],
            device_id=(dp, lax.rem(me + 1, n_sp)), device_id_type=MESH)

    def send_edge(s, layer):
        for first, end, rows in groups:
            @pl.when((layer >= first) & (layer < end) & (me + 1 < n_sp))
            def _():
                edge_copy(s, layer, rows).start()

    def far_copy(s, piece):
        rows = span // PIECES
        return pltpu.make_async_remote_copy(
            src_ref=u.at[s, last, pl.ds(span + piece * rows, rows)],
            dst_ref=u.at[s, last, pl.ds(piece * rows, rows)],
            send_sem=far_send_sem.at[s], recv_sem=far_recv_sem.at[s, piece // (PIECES // 2)],
            device_id=(dp, lax.rem(me + far_hops, n_sp)), device_id_type=MESH)

    sends_far = me + far_hops < n_sp

    sig_in = pltpu.make_async_copy(signal, u.at[:, 0, pl.ds(span, span)], sig_sem)
    cond_in = pltpu.make_async_copy(cond, c, cond_sem)
    bias_in = pltpu.make_async_copy(b_gate, bias, bias_sem)
    for copy in (sig_in, cond_in, bias_in):
        copy.start()
    for layer in range(AHEAD):
        start_weights(layer)

    barrier = pltpu.get_barrier_semaphore()
    for off in range(1, n_sp):
        pl.semaphore_signal(barrier, inc=1, device_id=(dp, lax.rem(me + off, n_sp)), device_id_type=MESH)

    @pl.when(me < 1)
    def _():
        for s in range(batch):
            for layer in range(last):
                u[s, layer, span - sizes[layer]:span] = jnp.zeros((sizes[layer], ch), BF16)

    @pl.when(me < far_hops)
    def _():
        for s in range(batch):
            u[s, last, :span] = jnp.zeros((span, ch), BF16)

    sig_in.wait()
    pl.semaphore_wait(barrier, n_sp - 1)
    for s in range(batch):
        send_edge(s, 0)
    for s in range(batch):
        h[s] = u[s, 0, span:].astype(F32)
    cond_in.wait()
    bias_in.wait()

    def gate(z):
        half = ch // 2
        parts = []
        for lo in (0, half):
            zf, zg = z(lo, lo + half), z(ch + lo, ch + lo + half)
            parts.append((jnp.tanh(zf) * (0.5 * jnp.tanh(0.5 * zg) + 0.5)).astype(BF16))
        return jnp.concatenate(parts, axis=1)

    def step(s, layer):
        @pl.when(s == 0)
        def _():
            @pl.when(layer < layers - AHEAD)
            def _():
                start_weights(layer + AHEAD)
            await_weights(layer)

        @pl.when((s == 1) & (layer == 1))
        def _():
            for k in range(layers):
                pltpu.make_async_copy(w_skip.at[k], w_sum.at[k], sum_sem).start()

        for first, end, rows in groups:
            @pl.when((layer >= first) & (layer < end) & (me >= 1))
            def _():
                edge_copy(s, layer, rows).wait_recv()

        dilation = jnp.left_shift(1, layer)

        def layer_body(past):
            x = jnp.concatenate([u[s, layer, span:], c[s], past], axis=1)
            a = gate(lambda lo, hi: jnp.dot(x, w_in[layer, :, lo:hi], preferred_element_type=F32) + bias[pl.ds(layer, 1), lo:hi])
            acts[s, layer] = a
            new_h = h[s] + jnp.dot(a, w_mix[layer], preferred_element_type=F32)
            h[s] = new_h
            u[s, layer + 1, span:] = new_h.astype(BF16)

        @pl.when(dilation < TILE)
        def _():
            wide = u[s, layer, span - TILE:].astype(F32)
            layer_body(pltpu.roll(wide, dilation, axis=0)[TILE:].astype(BF16))

        @pl.when(dilation >= TILE)
        def _():
            base = pl.multiple_of(span - jnp.minimum(dilation, span), TILE)
            layer_body(u[s, layer, pl.ds(base, span)])

        send_edge(s, layer + 1)

        @pl.when(sends_far)
        def _():
            @pl.when((s == 0) & (layer == last - 1))
            def _():
                far_copy(0, 0).start()

            @pl.when((s == 1) & (layer == 0))
            def _():
                for piece in range(1, PIECES - 5):
                    far_copy(0, piece).start()

            @pl.when((s == 1) & (layer >= 1) & (layer < 6))
            def _():
                far_copy(0, layer + PIECES - 6).start()

            @pl.when((s == 1) & (layer == last - 1))
            def _():
                for piece in range(PIECES):
                    far_copy(1, piece).start()

    def last_step(s):
        @pl.when(s == 0)
        def _():
            await_weights(last)

        near = jnp.concatenate([u[s, last, span:], c[s]], axis=1)
        depth = near.shape[1]
        z_part[...] = jnp.dot(near, w_in[last, :depth], preferred_element_type=F32) + bias[last:, :]

        rows = span // 2

        def finish(part, carry):
            at = pl.ds(pl.multiple_of(part * rows, rows), rows)

            @pl.when(me >= far_hops)
            def _():
                landed(u.at[s, last, at], far_recv_sem.at[s, part])

            past = u[s, last, at]
            a = gate(lambda lo, hi: z_part[at, lo:hi] + jnp.dot(past, w_in[last, depth:, lo:hi], preferred_element_type=F32))
            h[s, at] += jnp.dot(a, w_mix[last], preferred_element_type=F32)
            skip[s, at] += jnp.dot(a, w_sum[last], preferred_element_type=F32)
            return carry

        lax.fori_loop(0, 2, finish, 0)

    def sum_skip(s):
        @pl.when(s == 0)
        def _():
            landed(w_sum, sum_sem)

        x = jnp.concatenate([acts[s, k] for k in range(last)], axis=1)
        skip[s] = jnp.dot(x, w_sum[:last].reshape(last * ch, skip.shape[2]), preferred_element_type=F32)

    early = [2 * k for k in range(9)] + [2 * k + 1 for k in range(9)] + [20, 21, 18, 19]
    late = [0, 1] + [2 * k for k in range(1, 9)] + [2 * k + 1 for k in range(1, 8)] + [20, 18, 17, 21, 19]

    def run(i, carry):
        code = jnp.where(me < n_sp // 2, at_step(i, early), at_step(i, late))
        s, layer = code % batch, code // batch

        @pl.when(layer < last)
        def _():
            step(s, layer)

        @pl.when(layer == last)
        def _():
            last_step(s)

        @pl.when(layer == layers)
        def _():
            sum_skip(s)
        return carry

    lax.fori_loop(0, len(early), run, 0)

    parts = next(n for n in range(1, layers) if sum(sizes) % (n * TILE) == 0 and sum(sizes) <= n * span)
    for s in range(batch):
        @pl.when(me + 1 < n_sp)
        def _():
            landed(u.at[s, pl.ds(0, parts), pl.ds(0, sum(sizes) // parts)], send_sem.at[s])

        @pl.when(sends_far)
        def _():
            landed(u.at[s, last, pl.ds(0, span)], far_send_sem.at[s])


def store_kernel(h, skip, h_out, skip_out, sem):
    copies = [pltpu.make_async_copy(h, h_out, sem.at[0]), pltpu.make_async_copy(skip, skip_out, sem.at[1])]
    for copy in copies:
        copy.start()
    for copy in copies:
        copy.wait()


def solution(mesh):
    n_sp = mesh.shape['sp']

    def local_stack(signal, cond_feats, w_now, w_past, w_cond, b_gate, w_res, w_skip):
        batch, span, ch = signal.shape
        layers, cond_ch, skip_ch = w_now.shape[0], cond_feats.shape[2], w_skip.shape[2]
        in_vmem = pl.BlockSpec(memory_space=pltpu.VMEM)
        h, skip = pl.pallas_call(
            functools.partial(stack_kernel, n_sp),
            out_shape=[pltpu.VMEM((batch, span, ch), F32), pltpu.VMEM((batch, span, skip_ch), F32)],
            in_specs=[pl.BlockSpec(memory_space=pltpu.HBM)] * 8,
            out_specs=[in_vmem] * 2,
            scratch_shapes=[
                pltpu.VMEM((batch, layers, 2 * span, ch), BF16),
                pltpu.VMEM((batch, layers - 1, span, ch), BF16),
                pltpu.VMEM((span, 2 * ch), F32),
                pltpu.VMEM((batch, span, cond_ch), BF16),
                pltpu.VMEM((layers, 2 * ch), F32),
                pltpu.VMEM((layers, 2 * ch + cond_ch, 2 * ch), BF16),
                pltpu.VMEM((layers, ch, ch), BF16),
                pltpu.VMEM((layers, ch, skip_ch), BF16),
                pltpu.SemaphoreType.DMA,
                pltpu.SemaphoreType.DMA,
                pltpu.SemaphoreType.DMA,
                pltpu.SemaphoreType.DMA((AHEAD + 1, 2)),
                pltpu.SemaphoreType.DMA,
                pltpu.SemaphoreType.DMA((batch,)),
                pltpu.SemaphoreType.DMA((batch, layers - 1)),
                pltpu.SemaphoreType.DMA((batch,)),
                pltpu.SemaphoreType.DMA((batch, 2)),
            ],
            compiler_params=pltpu.CompilerParams(collective_id=0, has_side_effects=True, vmem_limit_bytes=60 * 2 ** 20),
        )(signal, cond_feats, w_now, w_past, w_cond, b_gate, w_res, w_skip)
        return pl.pallas_call(
            store_kernel,
            out_shape=[jax.ShapeDtypeStruct((batch, span, ch), F32), jax.ShapeDtypeStruct((batch, span, skip_ch), F32)],
            in_specs=[in_vmem] * 2,
            out_specs=[pl.BlockSpec(memory_space=pl.ANY)] * 2,
            scratch_shapes=[pltpu.SemaphoreType.DMA((2,))],
            compiler_params=pltpu.CompilerParams(vmem_limit_bytes=2 ** 20),
        )(h, skip)

    seq_spec = P('dp', 'sp', None)
    return jax.shard_map(local_stack, mesh=mesh,
                         in_specs=(seq_spec, seq_spec, P(), P(), P(), P(), P(), P()),
                         out_specs=(seq_spec, seq_spec), check_vma=False)
```

```python
import functools

import jax
import jax.numpy as jnp
from jax import lax
from jax.experimental import pallas as pl
from jax.experimental.pallas import tpu as pltpu
from jax.sharding import PartitionSpec as P

BF16, F32 = jnp.bfloat16, jnp.float32
MESH = pl.DeviceIdType.MESH
TILE = 16
AHEAD = 2
PIECES = 8


def at_step(i, order):
    code = 2 * i + (order[-1] - 2 * (len(order) - 1))
    for j in range(len(order) - 2, -1, -1):
        if order[j] - 2 * j != order[j + 1] - 2 * (j + 1):
            code = jnp.where(i <= j, 2 * i + (order[j] - 2 * j), code)
    return code


def stack_kernel(n_sp, signal, cond, w_now, w_past, w_cond, b_gate, w_res, w_skip, h_out, skip,
                 u, h, acts, z_part, c, bias, w_in, w_mix, w_sum,
                 sig_sem, cond_sem, bias_sem, w_sem, sum_sem, send_sem, recv_sem, far_send_sem, far_recv_sem,
                 cond_send_sem, cond_recv_sem):
    batch, layers, span, ch = u.shape[0], w_in.shape[0], h_out.shape[1], h_out.shape[2]
    last, cond_ch = layers - 1, c.shape[2]
    dp, me = lax.axis_index('dp'), lax.axis_index('sp')

    near = next(k for k in range(layers) if 2 ** k >= TILE)
    sizes = {k: min(max(TILE, 2 ** k), span) for k in range(last) if k == 0 or k >= near}
    far_hops = 2 ** last // span

    def start_weights(layer):
        slot = lax.rem(layer, AHEAD + 1)
        for src, dst in ((w_now.at[layer], w_in.at[layer, pl.ds(0, ch)]),
                         (w_cond.at[layer], w_in.at[layer, pl.ds(ch, cond_ch)]),
                         (w_past.at[layer], w_in.at[layer, pl.ds(ch + cond_ch, ch)])):
            pltpu.make_async_copy(src, dst, w_sem.at[slot, 0]).start()
        pltpu.make_async_copy(w_res.at[layer], w_mix.at[layer], w_sem.at[slot, 1]).start()

    def landed(ref, sem):
        pltpu.make_async_copy(ref, ref, sem).wait()

    def await_weights(layer):
        slot = lax.rem(layer, AHEAD + 1)
        landed(w_in.at[layer], w_sem.at[slot, 0])
        landed(w_mix.at[layer], w_sem.at[slot, 1])

    def edge_copy(s, layer, rows):
        return pltpu.make_async_remote_copy(
            src_ref=u.at[s, layer, pl.ds(2 * span - rows, rows)],
            dst_ref=u.at[s, layer, pl.ds(span - rows, rows)],
            send_sem=send_sem.at[s], recv_sem=recv_sem.at[s, layer],
            device_id=(dp, lax.rem(me + 1, n_sp)), device_id_type=MESH)

    def send_edge(s, layer):
        for k, rows in sizes.items():
            @pl.when((layer == k) & (me + 1 < n_sp))
            def _():
                edge_copy(s, k, rows).start()

    def cond_copy(s):
        return pltpu.make_async_remote_copy(
            src_ref=c.at[s, pl.ds(span, TILE)], dst_ref=c.at[s, pl.ds(0, TILE)],
            send_sem=cond_send_sem, recv_sem=cond_recv_sem.at[s],
            device_id=(dp, lax.rem(me + 1, n_sp)), device_id_type=MESH)

    def far_copy(s, piece):
        rows = span // PIECES
        return pltpu.make_async_remote_copy(
            src_ref=u.at[s, last, pl.ds(span + piece * rows, rows)],
            dst_ref=u.at[s, last, pl.ds(piece * rows, rows)],
            send_sem=far_send_sem.at[s], recv_sem=far_recv_sem.at[s, piece // (PIECES // 2)],
            device_id=(dp, lax.rem(me + far_hops, n_sp)), device_id_type=MESH)

    sends_far = me + far_hops < n_sp

    sig_in = pltpu.make_async_copy(signal, u.at[:, 0, pl.ds(span, span)], sig_sem)
    cond_in = pltpu.make_async_copy(cond, c.at[:, pl.ds(TILE, span)], cond_sem)
    bias_in = pltpu.make_async_copy(b_gate, bias, bias_sem)
    for copy in (sig_in, cond_in, bias_in):
        copy.start()
    start_weights(0)

    barrier = pltpu.get_barrier_semaphore()
    chip = n_sp // 2
    partner = me + 1 - 2 * lax.rem(me, 2)
    pl.semaphore_signal(barrier, inc=1, device_id=(dp, partner), device_id_type=MESH)

    def greet_other_chip():
        for core in range(chip):
            pl.semaphore_signal(barrier, inc=1, device_id=(dp, (1 - me // chip) * chip + core), device_id_type=MESH)

    @pl.when(me < 1)
    def _():
        for s in range(batch):
            for layer, rows in sizes.items():
                u[s, layer, span - rows:span] = jnp.zeros((rows, ch), BF16)

    @pl.when(me < far_hops)
    def _():
        for s in range(batch):
            u[s, last, :span] = jnp.zeros((span, ch), BF16)

    @pl.when(me < chip)
    def _():
        pl.semaphore_wait(barrier, 1)
        greet_other_chip()

    @pl.when(me >= chip)
    def _():
        pl.semaphore_wait(barrier, n_sp - 1)
        greet_other_chip()

    sig_in.wait()
    for layer in range(1, AHEAD):
        start_weights(layer)
    cond_in.wait()

    def send_first():
        for s in range(batch):
            edge_copy(s, 0, sizes[0]).start()
            cond_copy(s).start()

    @pl.when(me == chip - 1)
    def _():
        pl.semaphore_wait(barrier, chip)

    @pl.when(me + 1 < n_sp)
    def _():
        send_first()

    for s in range(batch):
        h[s, TILE:] = u[s, 0, span:].astype(F32)
        h[s, :TILE] = jnp.zeros((TILE, ch), F32)
    bias_in.wait()

    def gate(z):
        half = ch // 2
        parts = []
        for lo in (0, half):
            zf, zg = z(lo, lo + half), z(ch + lo, ch + lo + half)
            parts.append((jnp.tanh(zf) * (0.5 * jnp.tanh(0.5 * zg) + 0.5)).astype(BF16))
        return jnp.concatenate(parts, axis=1)

    def step(s, layer):
        @pl.when(s == 0)
        def _():
            await_weights(layer)

            @pl.when(layer < layers - AHEAD)
            def _():
                start_weights(layer + AHEAD)

        @pl.when((s == 0) & (layer == last - 2))
        def _():
            for k in range(layers):
                pltpu.make_async_copy(w_skip.at[k], w_sum.at[k], sum_sem).start()

        for k, rows in sizes.items():
            @pl.when((layer == k) & (me >= 1))
            def _():
                edge_copy(s, k, rows).wait_recv()
                if k == 0:
                    cond_copy(s).wait_recv()
                    h[s, :TILE] = u[s, 0, span - TILE:span].astype(F32)

        dilation = jnp.left_shift(1, layer)

        def layer_body(ahead, past):
            x = jnp.concatenate([u[s, layer, span - ahead:], c[s, TILE - ahead:], past], axis=1)
            a = gate(lambda lo, hi: jnp.dot(x, w_in[layer, :, lo:hi], preferred_element_type=F32) + bias[pl.ds(layer, 1), lo:hi])
            acts[s, layer] = a[ahead:]
            new_h = h[s, TILE - ahead:] + jnp.dot(a, w_mix[layer], preferred_element_type=F32)
            h[s, TILE - ahead:] = new_h
            new_u = new_h.astype(BF16)
            u[s, layer + 1, span:] = new_u[ahead:]
            return new_u[:ahead]

        @pl.when(layer < near)
        def _():
            wide = u[s, layer, span - 2 * TILE:].astype(F32)
            edge = layer_body(TILE, pltpu.roll(wide, dilation, axis=0)[TILE:].astype(BF16))

            @pl.when(layer + 1 < near)
            def _():
                u[s, layer + 1, span - TILE:span] = jnp.where(me > 0, edge, jnp.zeros_like(edge))

        @pl.when(layer >= near)
        def _():
            base = pl.multiple_of(span - jnp.minimum(dilation, span), TILE)
            layer_body(0, u[s, layer, pl.ds(base, span)])

        @pl.when((s == 0) & (layer == 0) & (me < chip - 1))
        def _():
            pl.semaphore_wait(barrier, chip)

        send_edge(s, layer + 1)

        @pl.when(sends_far)
        def _():
            @pl.when((s == 0) & (layer == last - 1))
            def _():
                far_copy(0, 0).start()

            @pl.when((s == 1) & (layer == 0))
            def _():
                for piece in range(1, PIECES - 5):
                    far_copy(0, piece).start()

            @pl.when((s == 1) & (layer >= 1) & (layer < 6))
            def _():
                far_copy(0, layer + PIECES - 6).start()

            @pl.when((s == 1) & (layer == last - 1))
            def _():
                for piece in range(PIECES):
                    far_copy(1, piece).start()

    def last_step(s):
        @pl.when(s == 0)
        def _():
            await_weights(last)

        x = jnp.concatenate([u[s, last, span:], c[s, TILE:]], axis=1)
        depth = x.shape[1]
        z_part[...] = jnp.dot(x, w_in[last, :depth], preferred_element_type=F32) + bias[last:, :]

        rows = span // 2

        def finish(part, carry):
            at = pl.ds(pl.multiple_of(part * rows, rows), rows)

            @pl.when(me >= far_hops)
            def _():
                landed(u.at[s, last, at], far_recv_sem.at[s, part])

            past = u[s, last, at]
            a = gate(lambda lo, hi: z_part[at, lo:hi] + jnp.dot(past, w_in[last, depth:, lo:hi], preferred_element_type=F32))
            h_out[s, at] = h[s, pl.ds(pl.multiple_of(TILE + part * rows, TILE), rows)] + jnp.dot(a, w_mix[last], preferred_element_type=F32)
            skip[s, at] += jnp.dot(a, w_sum[last], preferred_element_type=F32)
            return carry

        lax.fori_loop(0, 2, finish, 0)

    def sum_skip(s):
        @pl.when(s == 0)
        def _():
            landed(w_sum, sum_sem)

        x = jnp.concatenate([acts[s, k] for k in range(last)], axis=1)
        skip[s] = jnp.dot(x, w_sum[:last].reshape(last * ch, skip.shape[2]), preferred_element_type=F32)

    early = [2 * k for k in range(9)] + [2 * k + 1 for k in range(9)] + [20, 21, 18, 19]
    late = [0, 2, 4, 6, 1, 3, 5, 7] + [2 * k for k in range(4, 9)] + [20] + [2 * k + 1 for k in range(4, 8)] + [18, 17, 21, 19]

    def run(i, carry):
        code = jnp.where(me < n_sp // 2, at_step(i, early), at_step(i, late))
        s, layer = code % batch, code // batch

        @pl.when(layer < last)
        def _():
            step(s, layer)

        @pl.when(layer == last)
        def _():
            last_step(s)

        @pl.when(layer == layers)
        def _():
            sum_skip(s)
        return carry

    lax.fori_loop(0, len(early), run, 0)

    total = sum(sizes.values())
    parts = next(n for n in range(1, layers) if total % (n * TILE) == 0 and total <= n * 2 * span)
    for s in range(batch):
        @pl.when(me + 1 < n_sp)
        def _():
            landed(u.at[s, pl.ds(0, parts), pl.ds(0, total // parts)], send_sem.at[s])

        @pl.when(sends_far)
        def _():
            landed(u.at[s, last, pl.ds(0, span)], far_send_sem.at[s])

    @pl.when(me + 1 < n_sp)
    def _():
        landed(c.at[:, pl.ds(span, TILE)], cond_send_sem)


def store_kernel(h, skip, h_out, skip_out, sem):
    copies = [pltpu.make_async_copy(h, h_out, sem.at[0]), pltpu.make_async_copy(skip, skip_out, sem.at[1])]
    for copy in copies:
        copy.start()
    for copy in copies:
        copy.wait()


def solution(mesh):
    n_sp = mesh.shape['sp']

    def local_stack(signal, cond_feats, w_now, w_past, w_cond, b_gate, w_res, w_skip):
        batch, span, ch = signal.shape
        layers, cond_ch, skip_ch = w_now.shape[0], cond_feats.shape[2], w_skip.shape[2]
        in_vmem = pl.BlockSpec(memory_space=pltpu.VMEM)
        h, skip = pl.pallas_call(
            functools.partial(stack_kernel, n_sp),
            out_shape=[pltpu.VMEM((batch, span, ch), F32), pltpu.VMEM((batch, span, skip_ch), F32)],
            in_specs=[pl.BlockSpec(memory_space=pltpu.HBM)] * 8,
            out_specs=[in_vmem] * 2,
            scratch_shapes=[
                pltpu.VMEM((batch, layers, 2 * span, ch), BF16),
                pltpu.VMEM((batch, span + TILE, ch), F32),
                pltpu.VMEM((batch, layers - 1, span, ch), BF16),
                pltpu.VMEM((span, 2 * ch), F32),
                pltpu.VMEM((batch, span + TILE, cond_ch), BF16),
                pltpu.VMEM((layers, 2 * ch), F32),
                pltpu.VMEM((layers, 2 * ch + cond_ch, 2 * ch), BF16),
                pltpu.VMEM((layers, ch, ch), BF16),
                pltpu.VMEM((layers, ch, skip_ch), BF16),
                pltpu.SemaphoreType.DMA,
                pltpu.SemaphoreType.DMA,
                pltpu.SemaphoreType.DMA,
                pltpu.SemaphoreType.DMA((AHEAD + 1, 2)),
                pltpu.SemaphoreType.DMA,
                pltpu.SemaphoreType.DMA((batch,)),
                pltpu.SemaphoreType.DMA((batch, layers - 1)),
                pltpu.SemaphoreType.DMA((batch,)),
                pltpu.SemaphoreType.DMA((batch, 2)),
                pltpu.SemaphoreType.DMA,
                pltpu.SemaphoreType.DMA((batch,)),
            ],
            compiler_params=pltpu.CompilerParams(collective_id=0, has_side_effects=True, vmem_limit_bytes=60 * 2 ** 20),
        )(signal, cond_feats, w_now, w_past, w_cond, b_gate, w_res, w_skip)
        return pl.pallas_call(
            store_kernel,
            out_shape=[jax.ShapeDtypeStruct((batch, span, ch), F32), jax.ShapeDtypeStruct((batch, span, skip_ch), F32)],
            in_specs=[in_vmem] * 2,
            out_specs=[pl.BlockSpec(memory_space=pl.ANY)] * 2,
            scratch_shapes=[pltpu.SemaphoreType.DMA((2,))],
            compiler_params=pltpu.CompilerParams(vmem_limit_bytes=2 ** 20),
        )(h, skip)

    seq_spec = P('dp', 'sp', None)
    return jax.shard_map(local_stack, mesh=mesh,
                         in_specs=(seq_spec, seq_spec, P(), P(), P(), P(), P(), P()),
                         out_specs=(seq_spec, seq_spec), check_vma=False)
```

```python
import functools

import jax
import jax.numpy as jnp
from jax import lax
from jax.experimental import pallas as pl
from jax.experimental.pallas import tpu as pltpu
from jax.sharding import PartitionSpec as P

BF16, F32 = jnp.bfloat16, jnp.float32
MESH = pl.DeviceIdType.MESH
TILE = 16
AHEAD = 2
PIECES = 8


def at_step(i, order):
    code = 2 * i + (order[-1] - 2 * (len(order) - 1))
    for j in range(len(order) - 2, -1, -1):
        if order[j] - 2 * j != order[j + 1] - 2 * (j + 1):
            code = jnp.where(i <= j, 2 * i + (order[j] - 2 * j), code)
    return code


def stack_kernel(n_sp, signal, cond, w_now, w_past, w_cond, b_gate, w_res, w_skip, h_out, skip,
                 u, h, acts, z_part, c, bias, w_in, w_mix, w_sum,
                 sig_sem, cond_sem, bias_sem, w_sem, sum_sem, send_sem, recv_sem, far_send_sem, far_recv_sem,
                 cond_send_sem, cond_recv_sem):
    batch, layers, span, ch = u.shape[0], w_in.shape[0], h_out.shape[1], h_out.shape[2]
    last, cond_ch = layers - 1, c.shape[2]
    dp, me = lax.axis_index('dp'), lax.axis_index('sp')

    near = next(k for k in range(layers) if 2 ** k >= TILE)
    sizes = {k: min(max(TILE, 2 ** k), span) for k in range(last) if k == 0 or k >= near}
    far_hops = 2 ** last // span

    def start_weights(layer):
        slot = lax.rem(layer, AHEAD + 1)
        for src, dst in ((w_now.at[layer], w_in.at[layer, pl.ds(0, ch)]),
                         (w_cond.at[layer], w_in.at[layer, pl.ds(ch, cond_ch)]),
                         (w_past.at[layer], w_in.at[layer, pl.ds(ch + cond_ch, ch)])):
            pltpu.make_async_copy(src, dst, w_sem.at[slot, 0]).start()
        pltpu.make_async_copy(w_res.at[layer], w_mix.at[layer], w_sem.at[slot, 1]).start()

    def landed(ref, sem):
        pltpu.make_async_copy(ref, ref, sem).wait()

    def await_weights(layer):
        slot = lax.rem(layer, AHEAD + 1)
        landed(w_in.at[layer], w_sem.at[slot, 0])
        landed(w_mix.at[layer], w_sem.at[slot, 1])

    def edge_copy(s, layer, rows):
        return pltpu.make_async_remote_copy(
            src_ref=u.at[s, layer, pl.ds(2 * span - rows, rows)],
            dst_ref=u.at[s, layer, pl.ds(span - rows, rows)],
            send_sem=send_sem.at[s], recv_sem=recv_sem.at[s, layer],
            device_id=(dp, lax.rem(me + 1, n_sp)), device_id_type=MESH)

    def pick(layer, layers, act):
        if len(layers) == 1:
            act(layers[0])
            return
        middle = len(layers) // 2
        lax.cond(layer < layers[middle],
                 lambda: pick(layer, layers[:middle], act), lambda: pick(layer, layers[middle:], act))

    exchanged = list(range(near, last))

    def cond_copy(s):
        return pltpu.make_async_remote_copy(
            src_ref=c.at[s, pl.ds(span, TILE)], dst_ref=c.at[s, pl.ds(0, TILE)],
            send_sem=cond_send_sem, recv_sem=cond_recv_sem.at[s],
            device_id=(dp, lax.rem(me + 1, n_sp)), device_id_type=MESH)

    def far_copy(s, piece):
        rows = span // PIECES
        return pltpu.make_async_remote_copy(
            src_ref=u.at[s, last, pl.ds(span + piece * rows, rows)],
            dst_ref=u.at[s, last, pl.ds(piece * rows, rows)],
            send_sem=far_send_sem.at[s], recv_sem=far_recv_sem.at[s, piece // (PIECES // 2)],
            device_id=(dp, lax.rem(me + far_hops, n_sp)), device_id_type=MESH)

    sends_far = me + far_hops < n_sp

    sig_in = pltpu.make_async_copy(signal, u.at[:, 0, pl.ds(span, span)], sig_sem)
    cond_in = pltpu.make_async_copy(cond, c.at[:, pl.ds(TILE, span)], cond_sem)
    bias_in = pltpu.make_async_copy(b_gate, bias, bias_sem)
    for copy in (sig_in, cond_in, bias_in):
        copy.start()
    start_weights(0)

    barrier = pltpu.get_barrier_semaphore()
    chip = n_sp // 2
    partner = me + 1 - 2 * lax.rem(me, 2)
    pl.semaphore_signal(barrier, inc=1, device_id=(dp, partner), device_id_type=MESH)

    def greet_other_chip():
        for core in range(chip):
            pl.semaphore_signal(barrier, inc=1, device_id=(dp, (1 - me // chip) * chip + core), device_id_type=MESH)

    @pl.when(me < 1)
    def _():
        for s in range(batch):
            for layer, rows in sizes.items():
                u[s, layer, span - rows:span] = jnp.zeros((rows, ch), BF16)

    @pl.when(me < far_hops)
    def _():
        for s in range(batch):
            u[s, last, :span] = jnp.zeros((span, ch), BF16)

    @pl.when(me < chip)
    def _():
        pl.semaphore_wait(barrier, 1)
        greet_other_chip()

    @pl.when(me >= chip)
    def _():
        pl.semaphore_wait(barrier, n_sp - 1)
        greet_other_chip()

    sig_in.wait()
    for layer in range(1, AHEAD):
        start_weights(layer)
    cond_in.wait()

    def send_first():
        for s in range(batch):
            edge_copy(s, 0, sizes[0]).start()
            cond_copy(s).start()

    @pl.when(me == chip - 1)
    def _():
        pl.semaphore_wait(barrier, chip)

    @pl.when(me + 1 < n_sp)
    def _():
        send_first()

    for s in range(batch):
        h[s, TILE:] = u[s, 0, span:].astype(F32)
        h[s, :TILE] = jnp.zeros((TILE, ch), F32)
    bias_in.wait()

    def gate(z):
        half = ch // 2
        parts = []
        for lo in (0, half):
            zf, zg = z(lo, lo + half), z(ch + lo, ch + lo + half)
            parts.append((jnp.tanh(zf) * (0.5 * jnp.tanh(0.5 * zg) + 0.5)).astype(BF16))
        return jnp.concatenate(parts, axis=1)

    def step(s, layer):
        @pl.when(s == 0)
        def _():
            await_weights(layer)

            @pl.when(layer < layers - AHEAD)
            def _():
                start_weights(layer + AHEAD)

            @pl.when(layer == last - 2)
            def _():
                for k in range(layers):
                    pltpu.make_async_copy(w_skip.at[k], w_sum.at[k], sum_sem).start()

        dilation = jnp.left_shift(1, layer)

        def layer_body(ahead, past):
            x = jnp.concatenate([u[s, layer, span - ahead:], c[s, TILE - ahead:], past], axis=1)
            a = gate(lambda lo, hi: jnp.dot(x, w_in[layer, :, lo:hi], preferred_element_type=F32) + bias[pl.ds(layer, 1), lo:hi])
            acts[s, layer] = a[ahead:]
            new_h = h[s, TILE - ahead:] + jnp.dot(a, w_mix[layer], preferred_element_type=F32)
            h[s, TILE - ahead:] = new_h
            new_u = new_h.astype(BF16)
            u[s, layer + 1, span:] = new_u[ahead:]
            return new_u[:ahead]

        def small():
            @pl.when((layer == 0) & (me >= 1))
            def _():
                edge_copy(s, 0, sizes[0]).wait_recv()
                cond_copy(s).wait_recv()
                h[s, :TILE] = u[s, 0, span - TILE:span].astype(F32)

            wide = u[s, layer, span - 2 * TILE:].astype(F32)
            edge = layer_body(TILE, pltpu.roll(wide, dilation, axis=0)[TILE:].astype(BF16))

            def keep_edge():
                u[s, layer + 1, span - TILE:span] = jnp.where(me > 0, edge, jnp.zeros_like(edge))

            def send():
                @pl.when(me + 1 < n_sp)
                def _():
                    edge_copy(s, near, sizes[near]).start()

            lax.cond(layer + 1 < near, keep_edge, send)

            @pl.when((layer == 0) & (s == 0) & (me < chip - 1))
            def _():
                pl.semaphore_wait(barrier, chip)

        def large():
            @pl.when(me >= 1)
            def _():
                pick(layer, exchanged, lambda k: edge_copy(s, k, sizes[k]).wait_recv())

            base = pl.multiple_of(span - jnp.minimum(dilation, span), TILE)
            layer_body(0, u[s, layer, pl.ds(base, span)])

            @pl.when((me + 1 < n_sp) & (layer + 1 < last))
            def _():
                pick(layer + 1, exchanged[1:], lambda k: edge_copy(s, k, sizes[k]).start())

        lax.cond(layer < near, small, large)

        @pl.when(sends_far)
        def _():
            def pieces(s, first, end):
                for piece in range(first, end):
                    far_copy(s, piece).start()

            def first_sequence():
                @pl.when(layer == last - 1)
                def _():
                    pieces(0, 0, 1)

            def second_sequence():
                pick(layer, list(range(last)), lambda k: (
                    pieces(0, 1, 3) if k == 0 else pieces(0, k + 2, k + 3) if k < 6
                    else pieces(1, 0, PIECES) if k == last - 1 else None))

            lax.cond(s == 0, first_sequence, second_sequence)

    def last_step(s):
        @pl.when(s == 0)
        def _():
            await_weights(last)

        x = jnp.concatenate([u[s, last, span:], c[s, TILE:]], axis=1)
        depth = x.shape[1]
        z_part[...] = jnp.dot(x, w_in[last, :depth], preferred_element_type=F32) + bias[last:, :]

        rows = span // 2

        def finish(part, carry):
            at = pl.ds(pl.multiple_of(part * rows, rows), rows)

            @pl.when(me >= far_hops)
            def _():
                landed(u.at[s, last, at], far_recv_sem.at[s, part])

            past = u[s, last, at]
            a = gate(lambda lo, hi: z_part[at, lo:hi] + jnp.dot(past, w_in[last, depth:, lo:hi], preferred_element_type=F32))
            h_out[s, at] = h[s, pl.ds(pl.multiple_of(TILE + part * rows, TILE), rows)] + jnp.dot(a, w_mix[last], preferred_element_type=F32)
            skip[s, at] += jnp.dot(a, w_sum[last], preferred_element_type=F32)
            return carry

        lax.fori_loop(0, 2, finish, 0)

    def sum_skip(s):
        @pl.when(s == 0)
        def _():
            landed(w_sum, sum_sem)

        x = jnp.concatenate([acts[s, k] for k in range(last)], axis=1)
        skip[s] = jnp.dot(x, w_sum[:last].reshape(last * ch, skip.shape[2]), preferred_element_type=F32)

    early = [2 * k for k in range(9)] + [2 * k + 1 for k in range(9)] + [20, 21, 18, 19]
    late = [0, 2, 4, 6, 1, 3, 5, 7] + [2 * k for k in range(4, 9)] + [20] + [2 * k + 1 for k in range(4, 8)] + [18, 17, 21, 19]

    def run(i, carry):
        code = jnp.where(me < n_sp // 2, at_step(i, early), at_step(i, late))
        s, layer = code % batch, code // batch

        lax.cond(layer < last, lambda: step(s, layer),
                 lambda: lax.cond(layer == last, lambda: last_step(s), lambda: sum_skip(s)))
        return carry

    lax.fori_loop(0, len(early), run, 0)

    total = sum(sizes.values())
    parts = next(n for n in range(1, layers) if total % (n * TILE) == 0 and total <= n * 2 * span)
    for s in range(batch):
        @pl.when(me + 1 < n_sp)
        def _():
            landed(u.at[s, pl.ds(0, parts), pl.ds(0, total // parts)], send_sem.at[s])

        @pl.when(sends_far)
        def _():
            landed(u.at[s, last, pl.ds(0, span)], far_send_sem.at[s])

    @pl.when(me + 1 < n_sp)
    def _():
        landed(c.at[:, pl.ds(span, TILE)], cond_send_sem)


def store_kernel(h, skip, h_out, skip_out, sem):
    copies = [pltpu.make_async_copy(h, h_out, sem.at[0]), pltpu.make_async_copy(skip, skip_out, sem.at[1])]
    for copy in copies:
        copy.start()
    for copy in copies:
        copy.wait()


def solution(mesh):
    n_sp = mesh.shape['sp']

    def local_stack(signal, cond_feats, w_now, w_past, w_cond, b_gate, w_res, w_skip):
        batch, span, ch = signal.shape
        layers, cond_ch, skip_ch = w_now.shape[0], cond_feats.shape[2], w_skip.shape[2]
        in_vmem = pl.BlockSpec(memory_space=pltpu.VMEM)
        h, skip = pl.pallas_call(
            functools.partial(stack_kernel, n_sp),
            out_shape=[pltpu.VMEM((batch, span, ch), F32), pltpu.VMEM((batch, span, skip_ch), F32)],
            in_specs=[pl.BlockSpec(memory_space=pltpu.HBM)] * 8,
            out_specs=[in_vmem] * 2,
            scratch_shapes=[
                pltpu.VMEM((batch, layers, 2 * span, ch), BF16),
                pltpu.VMEM((batch, span + TILE, ch), F32),
                pltpu.VMEM((batch, layers - 1, span, ch), BF16),
                pltpu.VMEM((span, 2 * ch), F32),
                pltpu.VMEM((batch, span + TILE, cond_ch), BF16),
                pltpu.VMEM((layers, 2 * ch), F32),
                pltpu.VMEM((layers, 2 * ch + cond_ch, 2 * ch), BF16),
                pltpu.VMEM((layers, ch, ch), BF16),
                pltpu.VMEM((layers, ch, skip_ch), BF16),
                pltpu.SemaphoreType.DMA,
                pltpu.SemaphoreType.DMA,
                pltpu.SemaphoreType.DMA,
                pltpu.SemaphoreType.DMA((AHEAD + 1, 2)),
                pltpu.SemaphoreType.DMA,
                pltpu.SemaphoreType.DMA((batch,)),
                pltpu.SemaphoreType.DMA((batch, layers - 1)),
                pltpu.SemaphoreType.DMA((batch,)),
                pltpu.SemaphoreType.DMA((batch, 2)),
                pltpu.SemaphoreType.DMA,
                pltpu.SemaphoreType.DMA((batch,)),
            ],
            compiler_params=pltpu.CompilerParams(collective_id=0, has_side_effects=True, vmem_limit_bytes=60 * 2 ** 20),
        )(signal, cond_feats, w_now, w_past, w_cond, b_gate, w_res, w_skip)
        return pl.pallas_call(
            store_kernel,
            out_shape=[jax.ShapeDtypeStruct((batch, span, ch), F32), jax.ShapeDtypeStruct((batch, span, skip_ch), F32)],
            in_specs=[in_vmem] * 2,
            out_specs=[pl.BlockSpec(memory_space=pl.ANY)] * 2,
            scratch_shapes=[pltpu.SemaphoreType.DMA((2,))],
            compiler_params=pltpu.CompilerParams(vmem_limit_bytes=2 ** 20),
        )(h, skip)

    seq_spec = P('dp', 'sp', None)
    return jax.shard_map(local_stack, mesh=mesh,
                         in_specs=(seq_spec, seq_spec, P(), P(), P(), P(), P(), P()),
                         out_specs=(seq_spec, seq_spec), check_vma=False)
```

```python
import functools

import jax
import jax.numpy as jnp
from jax import lax
from jax.experimental import pallas as pl
from jax.experimental.pallas import tpu as pltpu
from jax.sharding import PartitionSpec as P

BF16, F32 = jnp.bfloat16, jnp.float32
MESH = pl.DeviceIdType.MESH
TILE = 16
AHEAD = 2
PIECES = 8


def at_step(i, order):
    code = 2 * i + (order[-1] - 2 * (len(order) - 1))
    for j in range(len(order) - 2, -1, -1):
        if order[j] - 2 * j != order[j + 1] - 2 * (j + 1):
            code = jnp.where(i <= j, 2 * i + (order[j] - 2 * j), code)
    return code


def stack_kernel(n_sp, signal, cond, w_now, w_past, w_cond, b_gate, w_res, w_skip, h_out, skip,
                 u, h, acts, z_part, c, bias, w_in, w_mix, w_sum,
                 sig_sem, cond_sem, bias_sem, w_sem, sum_sem, send_sem, recv_sem, far_send_sem, far_recv_sem,
                 cond_send_sem, cond_recv_sem):
    batch, layers, span, ch = u.shape[0], w_in.shape[0], h_out.shape[1], h_out.shape[2]
    last, cond_ch = layers - 1, c.shape[2]
    dp, me = lax.axis_index('dp'), lax.axis_index('sp')

    near = next(k for k in range(layers) if 2 ** k >= TILE)
    sizes = {k: min(max(TILE, 2 ** k), span) for k in range(last) if k == 0 or k >= near}
    far_hops = 2 ** last // span

    def start_weights(layer):
        slot = lax.rem(layer, AHEAD + 1)
        for src, dst in ((w_now.at[layer], w_in.at[layer, pl.ds(0, ch)]),
                         (w_cond.at[layer], w_in.at[layer, pl.ds(ch, cond_ch)]),
                         (w_past.at[layer], w_in.at[layer, pl.ds(ch + cond_ch, ch)])):
            pltpu.make_async_copy(src, dst, w_sem.at[slot, 0]).start()
        pltpu.make_async_copy(w_res.at[layer], w_mix.at[layer], w_sem.at[slot, 1]).start()

    def landed(ref, sem):
        pltpu.make_async_copy(ref, ref, sem).wait()

    def await_weights(layer):
        slot = lax.rem(layer, AHEAD + 1)
        landed(w_in.at[layer], w_sem.at[slot, 0])
        landed(w_mix.at[layer], w_sem.at[slot, 1])

    def edge_copy(s, layer, rows):
        return pltpu.make_async_remote_copy(
            src_ref=u.at[s, layer, pl.ds(2 * span - rows, rows)],
            dst_ref=u.at[s, layer, pl.ds(span - rows, rows)],
            send_sem=send_sem.at[s], recv_sem=recv_sem.at[s, layer if layer < 1 else layer - near + 1],
            device_id=(dp, lax.rem(me + 1, n_sp)), device_id_type=MESH)

    def pick(layer, layers, act):
        if len(layers) == 1:
            act(layers[0])
            return
        middle = len(layers) // 2
        lax.cond(layer < layers[middle],
                 lambda: pick(layer, layers[:middle], act), lambda: pick(layer, layers[middle:], act))

    exchanged = list(range(near, last))

    def cond_copy(s):
        return pltpu.make_async_remote_copy(
            src_ref=c.at[s, pl.ds(span, TILE)], dst_ref=c.at[s, pl.ds(0, TILE)],
            send_sem=cond_send_sem, recv_sem=cond_recv_sem.at[s],
            device_id=(dp, lax.rem(me + 1, n_sp)), device_id_type=MESH)

    def far_copy(s, piece):
        rows = span // PIECES
        return pltpu.make_async_remote_copy(
            src_ref=u.at[s, last, pl.ds(span + piece * rows, rows)],
            dst_ref=u.at[s, last, pl.ds(piece * rows, rows)],
            send_sem=far_send_sem.at[s], recv_sem=far_recv_sem.at[s, piece // (PIECES // 2)],
            device_id=(dp, lax.rem(me + far_hops, n_sp)), device_id_type=MESH)

    sends_far = me + far_hops < n_sp

    sig_in = pltpu.make_async_copy(signal, u.at[:, 0, pl.ds(span, span)], sig_sem)
    cond_in = pltpu.make_async_copy(cond, c.at[:, pl.ds(TILE, span)], cond_sem)
    bias_in = pltpu.make_async_copy(b_gate, bias, bias_sem)
    for copy in (sig_in, cond_in, bias_in):
        copy.start()
    start_weights(0)

    barrier = pltpu.get_barrier_semaphore()
    chip = n_sp // 2
    partner = me + 1 - 2 * lax.rem(me, 2)
    pl.semaphore_signal(barrier, inc=1, device_id=(dp, partner), device_id_type=MESH)

    def greet_other_chip():
        for core in range(chip):
            pl.semaphore_signal(barrier, inc=1, device_id=(dp, (1 - me // chip) * chip + core), device_id_type=MESH)

    @pl.when(me < 1)
    def _():
        for s in range(batch):
            for layer, rows in sizes.items():
                u[s, layer, span - rows:span] = jnp.zeros((rows, ch), BF16)

    @pl.when(me < far_hops)
    def _():
        for s in range(batch):
            u[s, last, :span] = jnp.zeros((span, ch), BF16)

    @pl.when(me < chip)
    def _():
        pl.semaphore_wait(barrier, 1)
        greet_other_chip()

    @pl.when(me >= chip)
    def _():
        pl.semaphore_wait(barrier, n_sp - 1)
        greet_other_chip()

    for layer in range(1, AHEAD):
        start_weights(layer)
    sig_in.wait()
    cond_in.wait()

    def send_first():
        for s in range(batch):
            edge_copy(s, 0, sizes[0]).start()
            cond_copy(s).start()

    @pl.when(me == chip - 1)
    def _():
        pl.semaphore_wait(barrier, chip)

    @pl.when(me + 1 < n_sp)
    def _():
        send_first()

    for s in range(batch):
        h[s, TILE:] = u[s, 0, span:].astype(F32)
        h[s, :TILE] = jnp.zeros((TILE, ch), F32)
    bias_in.wait()

    def gate(z):
        half = ch // 2
        parts = []
        for lo in (0, half):
            zf, zg = z(lo, lo + half), z(ch + lo, ch + lo + half)
            parts.append((jnp.tanh(zf) * (0.5 * jnp.tanh(0.5 * zg) + 0.5)).astype(BF16))
        return jnp.concatenate(parts, axis=1)

    def step(s, layer):
        @pl.when(s == 0)
        def _():
            @pl.when(layer < layers - AHEAD)
            def _():
                start_weights(layer + AHEAD)

            await_weights(layer)

        dilation = jnp.left_shift(1, layer)

        def layer_body(ahead, past):
            x = jnp.concatenate([u[s, layer, span - ahead:], c[s, TILE - ahead:], past], axis=1)
            a = gate(lambda lo, hi: jnp.dot(x, w_in[layer, :, lo:hi], preferred_element_type=F32) + bias[pl.ds(layer, 1), lo:hi])
            acts[s, layer] = a[ahead:]
            new_h = h[s, TILE - ahead:] + jnp.dot(a, w_mix[layer], preferred_element_type=F32)
            h[s, TILE - ahead:] = new_h
            new_u = new_h.astype(BF16)
            u[s, layer + 1, span:] = new_u[ahead:]
            return new_u[:ahead]

        def small():
            @pl.when((layer == 0) & (me >= 1))
            def _():
                edge_copy(s, 0, sizes[0]).wait_recv()
                cond_copy(s).wait_recv()
                h[s, :TILE] = u[s, 0, span - TILE:span].astype(F32)

            wide = u[s, layer, span - 2 * TILE:].astype(F32)
            edge = layer_body(TILE, pltpu.roll(wide, dilation, axis=0)[TILE:].astype(BF16))

            def keep_edge():
                u[s, layer + 1, span - TILE:span] = jnp.where(me > 0, edge, jnp.zeros_like(edge))

            def send():
                @pl.when(me + 1 < n_sp)
                def _():
                    edge_copy(s, near, sizes[near]).start()

            lax.cond(layer + 1 < near, keep_edge, send)

            @pl.when((layer == 0) & (s == 0) & (me < chip - 1))
            def _():
                pl.semaphore_wait(barrier, chip)

        def large():
            @pl.when((s == 1) & (layer == near))
            def _():
                for k in range(layers):
                    pltpu.make_async_copy(w_skip.at[k], w_sum.at[k], sum_sem).start()

            @pl.when(me >= 1)
            def _():
                pick(layer, exchanged, lambda k: edge_copy(s, k, sizes[k]).wait_recv())

            base = pl.multiple_of(span - jnp.minimum(dilation, span), TILE)
            layer_body(0, u[s, layer, pl.ds(base, span)])

            @pl.when((me + 1 < n_sp) & (layer + 1 < last))
            def _():
                pick(layer + 1, exchanged[1:], lambda k: edge_copy(s, k, sizes[k]).start())

        lax.cond(layer < near, small, large)

        @pl.when(sends_far)
        def _():
            def pieces(s, first, end):
                for piece in range(first, end):
                    far_copy(s, piece).start()

            def first_sequence():
                @pl.when(layer == last - 1)
                def _():
                    pieces(0, 0, 1)

            def second_sequence():
                pick(layer, list(range(last)), lambda k: (
                    pieces(0, 1, 3) if k == 0 else pieces(0, k + 2, k + 3) if k < 6
                    else pieces(1, 0, PIECES) if k == last - 1 else None))

            lax.cond(s == 0, first_sequence, second_sequence)

    def last_step(s):
        @pl.when(s == 0)
        def _():
            await_weights(last)

        x = jnp.concatenate([u[s, last, span:], c[s, TILE:]], axis=1)
        depth = x.shape[1]
        z_part[...] = jnp.dot(x, w_in[last, :depth], preferred_element_type=F32) + bias[last:, :]

        rows = span // 2

        def finish(part, carry):
            at = pl.ds(pl.multiple_of(part * rows, rows), rows)

            @pl.when(me >= far_hops)
            def _():
                landed(u.at[s, last, at], far_recv_sem.at[s, part])

            past = u[s, last, at]
            a = gate(lambda lo, hi: z_part[at, lo:hi] + jnp.dot(past, w_in[last, depth:, lo:hi], preferred_element_type=F32))
            h_out[s, at] = h[s, pl.ds(pl.multiple_of(TILE + part * rows, TILE), rows)] + jnp.dot(a, w_mix[last], preferred_element_type=F32)
            skip[s, at] += jnp.dot(a, w_sum[last], preferred_element_type=F32)
            return carry

        lax.fori_loop(0, 2, finish, 0)

    def sum_skip(s):
        @pl.when(s == 0)
        def _():
            landed(w_sum, sum_sem)

        x = jnp.concatenate([acts[s, k] for k in range(last)], axis=1)
        skip[s] = jnp.dot(x, w_sum[:last].reshape(last * ch, skip.shape[2]), preferred_element_type=F32)

    early = [2 * k for k in range(9)] + [2 * k + 1 for k in range(9)] + [20, 21, 18, 19]
    late = [0, 2, 4, 6, 1, 3, 5, 7] + [2 * k for k in range(4, 9)] + [2 * k + 1 for k in range(4, 8)] + [20, 18, 17, 21, 19]

    def run(i, carry):
        code = jnp.where(me < n_sp // 2, at_step(i, early), at_step(i, late))
        s, layer = code % batch, code // batch

        lax.cond(layer < last, lambda: step(s, layer),
                 lambda: lax.cond(layer == last, lambda: last_step(s), lambda: sum_skip(s)))
        return carry

    lax.fori_loop(0, len(early), run, 0)

    total = sum(sizes.values())
    parts = next(n for n in range(1, layers) if total % (n * TILE) == 0 and total <= n * 2 * span)
    for s in range(batch):
        @pl.when(me + 1 < n_sp)
        def _():
            landed(u.at[s, pl.ds(0, parts), pl.ds(0, total // parts)], send_sem.at[s])

        @pl.when(sends_far)
        def _():
            landed(u.at[s, last, pl.ds(0, span)], far_send_sem.at[s])

    @pl.when(me + 1 < n_sp)
    def _():
        landed(c.at[:, pl.ds(span, TILE)], cond_send_sem)


def store_kernel(h, skip, h_out, skip_out, sem):
    copies = [pltpu.make_async_copy(h, h_out, sem.at[0]), pltpu.make_async_copy(skip, skip_out, sem.at[1])]
    for copy in copies:
        copy.start()
    for copy in copies:
        copy.wait()


def solution(mesh):
    n_sp = mesh.shape['sp']

    def local_stack(signal, cond_feats, w_now, w_past, w_cond, b_gate, w_res, w_skip):
        batch, span, ch = signal.shape
        layers, cond_ch, skip_ch = w_now.shape[0], cond_feats.shape[2], w_skip.shape[2]
        in_vmem = pl.BlockSpec(memory_space=pltpu.VMEM)
        h, skip = pl.pallas_call(
            functools.partial(stack_kernel, n_sp),
            out_shape=[pltpu.VMEM((batch, span, ch), F32), pltpu.VMEM((batch, span, skip_ch), F32)],
            in_specs=[pl.BlockSpec(memory_space=pltpu.HBM)] * 8,
            out_specs=[in_vmem] * 2,
            scratch_shapes=[
                pltpu.VMEM((batch, layers, 2 * span, ch), BF16),
                pltpu.VMEM((batch, span + TILE, ch), F32),
                pltpu.VMEM((batch, layers - 1, span, ch), BF16),
                pltpu.VMEM((span, 2 * ch), F32),
                pltpu.VMEM((batch, span + TILE, cond_ch), BF16),
                pltpu.VMEM((layers, 2 * ch), F32),
                pltpu.VMEM((layers, 2 * ch + cond_ch, 2 * ch), BF16),
                pltpu.VMEM((layers, ch, ch), BF16),
                pltpu.VMEM((layers, ch, skip_ch), BF16),
                pltpu.SemaphoreType.DMA,
                pltpu.SemaphoreType.DMA,
                pltpu.SemaphoreType.DMA,
                pltpu.SemaphoreType.DMA((AHEAD + 1, 2)),
                pltpu.SemaphoreType.DMA,
                pltpu.SemaphoreType.DMA((batch,)),
                pltpu.SemaphoreType.DMA((batch, 6)),
                pltpu.SemaphoreType.DMA((batch,)),
                pltpu.SemaphoreType.DMA((batch, 2)),
                pltpu.SemaphoreType.DMA,
                pltpu.SemaphoreType.DMA((batch,)),
            ],
            compiler_params=pltpu.CompilerParams(collective_id=0, has_side_effects=True, vmem_limit_bytes=60 * 2 ** 20),
        )(signal, cond_feats, w_now, w_past, w_cond, b_gate, w_res, w_skip)
        return pl.pallas_call(
            store_kernel,
            out_shape=[jax.ShapeDtypeStruct((batch, span, ch), F32), jax.ShapeDtypeStruct((batch, span, skip_ch), F32)],
            in_specs=[in_vmem] * 2,
            out_specs=[pl.BlockSpec(memory_space=pl.ANY)] * 2,
            scratch_shapes=[pltpu.SemaphoreType.DMA((2,))],
            compiler_params=pltpu.CompilerParams(vmem_limit_bytes=2 ** 20),
        )(h, skip)

    seq_spec = P('dp', 'sp', None)
    return jax.shard_map(local_stack, mesh=mesh,
                         in_specs=(seq_spec, seq_spec, P(), P(), P(), P(), P(), P()),
                         out_specs=(seq_spec, seq_spec), check_vma=False)
```

```python
import functools

import jax
import jax.numpy as jnp
from jax import lax
from jax.experimental import pallas as pl
from jax.experimental.pallas import tpu as pltpu
from jax.sharding import PartitionSpec as P

BF16, F32 = jnp.bfloat16, jnp.float32
MESH = pl.DeviceIdType.MESH
TILE = 16
AHEAD = 2
PIECES = 8


def at_step(i, order):
    code = 2 * i + (order[-1] - 2 * (len(order) - 1))
    for j in range(len(order) - 2, -1, -1):
        if order[j] - 2 * j != order[j + 1] - 2 * (j + 1):
            code = jnp.where(i <= j, 2 * i + (order[j] - 2 * j), code)
    return code


def stack_kernel(n_sp, signal, cond, w_now, w_past, w_cond, b_gate, w_res, w_skip, h_out, skip,
                 u, h, acts, z_part, c, bias, w_in, w_mix, w_sum,
                 sig_sem, cond_sem, bias_sem, w_sem, sum_sem, send_sem, recv_sem, far_send_sem, far_recv_sem,
                 cond_send_sem, cond_recv_sem):
    batch, layers, span, ch = u.shape[0], w_in.shape[0], h_out.shape[1], h_out.shape[2]
    last, cond_ch = layers - 1, c.shape[2]
    dp, me = lax.axis_index('dp'), lax.axis_index('sp')

    near = next(k for k in range(layers) if 2 ** k >= TILE)
    sizes = {k: min(max(TILE, 2 ** k), span) for k in range(last) if k == 0 or k >= near}
    far_hops = 2 ** last // span

    def start_weights(layer):
        slot = lax.rem(layer, AHEAD + 1)
        for src, dst in ((w_now.at[layer], w_in.at[layer, pl.ds(0, ch)]),
                         (w_cond.at[layer], w_in.at[layer, pl.ds(ch, cond_ch)]),
                         (w_past.at[layer], w_in.at[layer, pl.ds(ch + cond_ch, ch)])):
            pltpu.make_async_copy(src, dst, w_sem.at[slot, 0]).start()
        pltpu.make_async_copy(w_res.at[layer], w_mix.at[layer], w_sem.at[slot, 1]).start()

    def landed(ref, sem):
        pltpu.make_async_copy(ref, ref, sem).wait()

    def await_weights(layer):
        slot = lax.rem(layer, AHEAD + 1)
        landed(w_in.at[layer], w_sem.at[slot, 0])
        landed(w_mix.at[layer], w_sem.at[slot, 1])

    def edge_copy(s, layer, rows):
        return pltpu.make_async_remote_copy(
            src_ref=u.at[s, layer, pl.ds(2 * span - rows, rows)],
            dst_ref=u.at[s, layer, pl.ds(span - rows, rows)],
            send_sem=send_sem.at[s], recv_sem=recv_sem.at[s, layer if layer < 1 else layer - near + 1],
            device_id=(dp, lax.rem(me + 1, n_sp)), device_id_type=MESH)

    def pick(layer, layers, act):
        if len(layers) == 1:
            act(layers[0])
            return
        middle = len(layers) // 2
        lax.cond(layer < layers[middle],
                 lambda: pick(layer, layers[:middle], act), lambda: pick(layer, layers[middle:], act))

    exchanged = list(range(near, last))

    def cond_copy(s):
        return pltpu.make_async_remote_copy(
            src_ref=c.at[s, pl.ds(span, TILE)], dst_ref=c.at[s, pl.ds(0, TILE)],
            send_sem=cond_send_sem, recv_sem=cond_recv_sem.at[s],
            device_id=(dp, lax.rem(me + 1, n_sp)), device_id_type=MESH)

    def far_copy(s, piece):
        rows = span // PIECES
        return pltpu.make_async_remote_copy(
            src_ref=u.at[s, last, pl.ds(span + piece * rows, rows)],
            dst_ref=u.at[s, last, pl.ds(piece * rows, rows)],
            send_sem=far_send_sem.at[s], recv_sem=far_recv_sem.at[s, piece // (PIECES // 2)],
            device_id=(dp, lax.rem(me + far_hops, n_sp)), device_id_type=MESH)

    sends_far = me + far_hops < n_sp

    sig_in = pltpu.make_async_copy(signal, u.at[:, 0, pl.ds(span, span)], sig_sem)
    cond_in = pltpu.make_async_copy(cond, c.at[:, pl.ds(TILE, span)], cond_sem)
    bias_in = pltpu.make_async_copy(b_gate, bias, bias_sem)
    for copy in (sig_in, cond_in, bias_in):
        copy.start()
    start_weights(0)

    barrier = pltpu.get_barrier_semaphore()
    chip = n_sp // 2
    partner = me + 1 - 2 * lax.rem(me, 2)
    pl.semaphore_signal(barrier, inc=1, device_id=(dp, partner), device_id_type=MESH)

    def greet_other_chip():
        for core in range(chip):
            pl.semaphore_signal(barrier, inc=1, device_id=(dp, (1 - me // chip) * chip + core), device_id_type=MESH)

    @pl.when(me < 1)
    def _():
        for s in range(batch):
            for layer, rows in sizes.items():
                u[s, layer, span - rows:span] = jnp.zeros((rows, ch), BF16)

    @pl.when(me < far_hops)
    def _():
        for s in range(batch):
            u[s, last, :span] = jnp.zeros((span, ch), BF16)

    @pl.when(me < chip)
    def _():
        pl.semaphore_wait(barrier, 1)
        greet_other_chip()

    @pl.when(me >= chip)
    def _():
        pl.semaphore_wait(barrier, n_sp - 1)
        greet_other_chip()

    for layer in range(1, AHEAD):
        start_weights(layer)
    sig_in.wait()
    cond_in.wait()

    def send_first():
        for s in range(batch):
            edge_copy(s, 0, sizes[0]).start()
            cond_copy(s).start()

    @pl.when(me == chip - 1)
    def _():
        pl.semaphore_wait(barrier, chip)

    @pl.when(me + 1 < n_sp)
    def _():
        send_first()

    for s in range(batch):
        h[s, TILE:] = u[s, 0, span:].astype(F32)
        h[s, :TILE] = jnp.zeros((TILE, ch), F32)
    bias_in.wait()

    def gate(z):
        half = ch // 2
        parts = []
        for lo in (0, half):
            zf, zg = z(lo, lo + half), z(ch + lo, ch + lo + half)
            parts.append((jnp.tanh(zf) * (0.5 * jnp.tanh(0.5 * zg) + 0.5)).astype(BF16))
        return jnp.concatenate(parts, axis=1)

    def step(s, layer):
        @pl.when(s == 0)
        def _():
            @pl.when(layer < layers - AHEAD)
            def _():
                start_weights(layer + AHEAD)

            await_weights(layer)

        dilation = jnp.left_shift(1, layer)

        def layer_body(ahead, past):
            x = jnp.concatenate([u[s, layer, span - ahead:], c[s, TILE - ahead:], past], axis=1)
            a = gate(lambda lo, hi: jnp.dot(x, w_in[layer, :, lo:hi], preferred_element_type=F32) + bias[pl.ds(layer, 1), lo:hi])
            acts[s, layer] = a[ahead:]
            new_h = h[s, TILE - ahead:] + jnp.dot(a, w_mix[layer], preferred_element_type=F32)
            h[s, TILE - ahead:] = new_h
            new_u = new_h.astype(BF16)
            u[s, layer + 1, span:] = new_u[ahead:]
            return new_u[:ahead]

        def small():
            @pl.when((layer == 0) & (me >= 1))
            def _():
                edge_copy(s, 0, sizes[0]).wait_recv()
                cond_copy(s).wait_recv()
                h[s, :TILE] = u[s, 0, span - TILE:span].astype(F32)

            wide = u[s, layer, span - 2 * TILE:].astype(F32)
            edge = layer_body(TILE, pltpu.roll(wide, dilation, axis=0)[TILE:].astype(BF16))

            def keep_edge():
                u[s, layer + 1, span - TILE:span] = jnp.where(me > 0, edge, jnp.zeros_like(edge))

            def send():
                @pl.when(me + 1 < n_sp)
                def _():
                    edge_copy(s, near, sizes[near]).start()

            lax.cond(layer + 1 < near, keep_edge, send)

            @pl.when((layer == 0) & (s == 0) & (me < chip - 1))
            def _():
                pl.semaphore_wait(barrier, chip)

        def large():
            @pl.when((s == 1) & (layer == near))
            def _():
                for k in range(layers):
                    pltpu.make_async_copy(w_skip.at[k], w_sum.at[k], sum_sem).start()

            @pl.when(me >= 1)
            def _():
                pick(layer, exchanged, lambda k: edge_copy(s, k, sizes[k]).wait_recv())

            base = pl.multiple_of(span - jnp.minimum(dilation, span), TILE)
            layer_body(0, u[s, layer, pl.ds(base, span)])

            @pl.when((me + 1 < n_sp) & (layer + 1 < last))
            def _():
                pick(layer + 1, exchanged[1:], lambda k: edge_copy(s, k, sizes[k]).start())

        lax.cond(layer < near, small, large)

        @pl.when(sends_far)
        def _():
            def pieces(s, first, end):
                for piece in range(first, end):
                    far_copy(s, piece).start()

            def first_sequence():
                @pl.when(layer == last - 1)
                def _():
                    pieces(0, 0, 1)

            def second_sequence():
                pick(layer, list(range(last)), lambda k: (
                    pieces(0, 1, 3) if k == 0 else pieces(0, k + 2, k + 3) if k < 6
                    else pieces(1, 0, PIECES) if k == last - 1 else None))

            lax.cond(s == 0, first_sequence, second_sequence)

    def last_step(s):
        @pl.when(s == 0)
        def _():
            await_weights(last)

        x = jnp.concatenate([u[s, last, span:], c[s, TILE:]], axis=1)
        depth = x.shape[1]
        z_part[...] = jnp.dot(x, w_in[last, :depth], preferred_element_type=F32) + bias[last:, :]

        rows = span // 2

        def finish(part, carry):
            at = pl.ds(pl.multiple_of(part * rows, rows), rows)

            @pl.when(me >= far_hops)
            def _():
                landed(u.at[s, last, at], far_recv_sem.at[s, part])

            past = u[s, last, at]
            a = gate(lambda lo, hi: z_part[at, lo:hi] + jnp.dot(past, w_in[last, depth:, lo:hi], preferred_element_type=F32))
            h_out[s, at] = h[s, pl.ds(pl.multiple_of(TILE + part * rows, TILE), rows)] + jnp.dot(a, w_mix[last], preferred_element_type=F32)
            x = jnp.concatenate([acts[s, last - 1, at], a], axis=1)
            skip[s, at] += jnp.dot(x, w_sum[last - 1:].reshape(2 * ch, skip.shape[2]), preferred_element_type=F32)
            return carry

        lax.fori_loop(0, 2, finish, 0, unroll=True)

    def sum_skip(s):
        @pl.when(s == 0)
        def _():
            landed(w_sum, sum_sem)

        x = jnp.concatenate([acts[s, k] for k in range(last - 1)], axis=1)
        skip[s] = jnp.dot(x, w_sum[:last - 1].reshape((last - 1) * ch, skip.shape[2]), preferred_element_type=F32)

    early = [2 * k for k in range(9)] + [2 * k + 1 for k in range(9)] + [20, 21, 18, 19]
    late = [0, 2, 4, 6, 1, 3, 5, 7] + [2 * k for k in range(4, 9)] + [2 * k + 1 for k in range(4, 8)] + [20, 18, 21, 17, 19]

    def run(i, carry):
        code = jnp.where(me < n_sp // 2, at_step(i, early), at_step(i, late))
        s, layer = code % batch, code // batch

        lax.cond(layer < last, lambda: step(s, layer),
                 lambda: lax.cond(layer == last, lambda: last_step(s), lambda: sum_skip(s)))
        return carry

    lax.fori_loop(0, len(early), run, 0)

    total = sum(sizes.values())
    parts = next(n for n in range(1, layers) if total % (n * TILE) == 0 and total <= n * 2 * span)
    for s in range(batch):
        @pl.when(me + 1 < n_sp)
        def _():
            landed(u.at[s, pl.ds(0, parts), pl.ds(0, total // parts)], send_sem.at[s])

        @pl.when(sends_far)
        def _():
            landed(u.at[s, last, pl.ds(0, span)], far_send_sem.at[s])

    @pl.when(me + 1 < n_sp)
    def _():
        landed(c.at[:, pl.ds(span, TILE)], cond_send_sem)


def store_kernel(h, skip, h_out, skip_out, sem):
    copies = [pltpu.make_async_copy(h, h_out, sem.at[0]), pltpu.make_async_copy(skip, skip_out, sem.at[1])]
    for copy in copies:
        copy.start()
    for copy in copies:
        copy.wait()


def solution(mesh):
    n_sp = mesh.shape['sp']

    def local_stack(signal, cond_feats, w_now, w_past, w_cond, b_gate, w_res, w_skip):
        batch, span, ch = signal.shape
        layers, cond_ch, skip_ch = w_now.shape[0], cond_feats.shape[2], w_skip.shape[2]
        in_vmem = pl.BlockSpec(memory_space=pltpu.VMEM)
        h, skip = pl.pallas_call(
            functools.partial(stack_kernel, n_sp),
            out_shape=[pltpu.VMEM((batch, span, ch), F32), pltpu.VMEM((batch, span, skip_ch), F32)],
            in_specs=[pl.BlockSpec(memory_space=pltpu.HBM)] * 8,
            out_specs=[in_vmem] * 2,
            scratch_shapes=[
                pltpu.VMEM((batch, layers, 2 * span, ch), BF16),
                pltpu.VMEM((batch, span + TILE, ch), F32),
                pltpu.VMEM((batch, layers - 1, span, ch), BF16),
                pltpu.VMEM((span, 2 * ch), F32),
                pltpu.VMEM((batch, span + TILE, cond_ch), BF16),
                pltpu.VMEM((layers, 2 * ch), F32),
                pltpu.VMEM((layers, 2 * ch + cond_ch, 2 * ch), BF16),
                pltpu.VMEM((layers, ch, ch), BF16),
                pltpu.VMEM((layers, ch, skip_ch), BF16),
                pltpu.SemaphoreType.DMA,
                pltpu.SemaphoreType.DMA,
                pltpu.SemaphoreType.DMA,
                pltpu.SemaphoreType.DMA((AHEAD + 1, 2)),
                pltpu.SemaphoreType.DMA,
                pltpu.SemaphoreType.DMA((batch,)),
                pltpu.SemaphoreType.DMA((batch, 6)),
                pltpu.SemaphoreType.DMA((batch,)),
                pltpu.SemaphoreType.DMA((batch, 2)),
                pltpu.SemaphoreType.DMA,
                pltpu.SemaphoreType.DMA((batch,)),
            ],
            compiler_params=pltpu.CompilerParams(collective_id=0, has_side_effects=True, vmem_limit_bytes=60 * 2 ** 20),
        )(signal, cond_feats, w_now, w_past, w_cond, b_gate, w_res, w_skip)
        return pl.pallas_call(
            store_kernel,
            out_shape=[jax.ShapeDtypeStruct((batch, span, ch), F32), jax.ShapeDtypeStruct((batch, span, skip_ch), F32)],
            in_specs=[in_vmem] * 2,
            out_specs=[pl.BlockSpec(memory_space=pl.ANY)] * 2,
            scratch_shapes=[pltpu.SemaphoreType.DMA((2,))],
            compiler_params=pltpu.CompilerParams(vmem_limit_bytes=2 ** 20),
        )(h, skip)

    seq_spec = P('dp', 'sp', None)
    return jax.shard_map(local_stack, mesh=mesh,
                         in_specs=(seq_spec, seq_spec, P(), P(), P(), P(), P(), P()),
                         out_specs=(seq_spec, seq_spec), check_vma=False)
```

```python
import functools

import jax
import jax.numpy as jnp
from jax import lax
from jax.experimental import pallas as pl
from jax.experimental.pallas import tpu as pltpu
from jax.sharding import PartitionSpec as P

BF16, F32 = jnp.bfloat16, jnp.float32
MESH = pl.DeviceIdType.MESH
TILE = 16
AHEAD = 2
PIECES = 8


def at_step(i, order):
    code = 2 * i + (order[-1] - 2 * (len(order) - 1))
    for j in range(len(order) - 2, -1, -1):
        if order[j] - 2 * j != order[j + 1] - 2 * (j + 1):
            code = jnp.where(i <= j, 2 * i + (order[j] - 2 * j), code)
    return code


def stack_kernel(n_sp, signal, cond, w_now, w_past, w_cond, b_gate, w_res, w_skip, h_out, skip,
                 u, h, acts, z_part, c, bias, w_in, w_mix, w_sum,
                 sig_sem, cond_sem, bias_sem, w_sem, sum_sem, send_sem, recv_sem, far_send_sem, far_recv_sem,
                 cond_send_sem, cond_recv_sem):
    batch, layers, span, ch = u.shape[0], w_in.shape[0], h_out.shape[1], h_out.shape[2]
    last, cond_ch = layers - 1, c.shape[2]
    dp, me = lax.axis_index('dp'), lax.axis_index('sp')

    near = next(k for k in range(layers) if 2 ** k >= TILE)
    sizes = {k: min(max(TILE, 2 ** k), span) for k in range(last) if k == 0 or k >= near}
    far_hops = 2 ** last // span

    def start_weights(layer):
        slot = lax.rem(layer, AHEAD + 1)
        for src, dst in ((w_now.at[layer], w_in.at[layer, pl.ds(0, ch)]),
                         (w_cond.at[layer], w_in.at[layer, pl.ds(ch, cond_ch)]),
                         (w_past.at[layer], w_in.at[layer, pl.ds(ch + cond_ch, ch)])):
            pltpu.make_async_copy(src, dst, w_sem.at[slot, 0]).start()
        pltpu.make_async_copy(w_res.at[layer], w_mix.at[layer], w_sem.at[slot, 1]).start()

    def landed(ref, sem):
        pltpu.make_async_copy(ref, ref, sem).wait()

    def await_weights(layer):
        slot = lax.rem(layer, AHEAD + 1)
        landed(w_in.at[layer], w_sem.at[slot, 0])
        landed(w_mix.at[layer], w_sem.at[slot, 1])

    def edge_copy(s, layer, rows):
        return pltpu.make_async_remote_copy(
            src_ref=u.at[s, layer, pl.ds(2 * span - rows, rows)],
            dst_ref=u.at[s, layer, pl.ds(span - rows, rows)],
            send_sem=send_sem.at[s], recv_sem=recv_sem.at[s, layer if layer < 1 else layer - near + 1],
            device_id=(dp, lax.rem(me + 1, n_sp)), device_id_type=MESH)

    def pick(layer, layers, act):
        if len(layers) == 1:
            act(layers[0])
            return
        middle = len(layers) // 2
        lax.cond(layer < layers[middle],
                 lambda: pick(layer, layers[:middle], act), lambda: pick(layer, layers[middle:], act))

    exchanged = list(range(near, last))

    def cond_copy(s):
        return pltpu.make_async_remote_copy(
            src_ref=c.at[s, pl.ds(span, TILE)], dst_ref=c.at[s, pl.ds(0, TILE)],
            send_sem=cond_send_sem, recv_sem=cond_recv_sem.at[s],
            device_id=(dp, lax.rem(me + 1, n_sp)), device_id_type=MESH)

    def far_copy(s, piece):
        rows = span // PIECES
        return pltpu.make_async_remote_copy(
            src_ref=u.at[s, last, pl.ds(span + piece * rows, rows)],
            dst_ref=u.at[s, last, pl.ds(piece * rows, rows)],
            send_sem=far_send_sem.at[s], recv_sem=far_recv_sem.at[s, piece // (PIECES // 2)],
            device_id=(dp, lax.rem(me + far_hops, n_sp)), device_id_type=MESH)

    sends_far = me + far_hops < n_sp

    sig_in = pltpu.make_async_copy(signal, u.at[:, 0, pl.ds(span, span)], sig_sem)
    cond_in = pltpu.make_async_copy(cond, c.at[:, pl.ds(TILE, span)], cond_sem)
    bias_in = pltpu.make_async_copy(b_gate, bias, bias_sem)
    for copy in (sig_in, cond_in, bias_in):
        copy.start()
    start_weights(0)

    barrier = pltpu.get_barrier_semaphore()
    chip = n_sp // 2
    partner = me + 1 - 2 * lax.rem(me, 2)
    pl.semaphore_signal(barrier, inc=1, device_id=(dp, partner), device_id_type=MESH)

    def greet_other_chip():
        for core in range(chip):
            pl.semaphore_signal(barrier, inc=1, device_id=(dp, (1 - me // chip) * chip + core), device_id_type=MESH)

    @pl.when(me < 1)
    def _():
        for s in range(batch):
            for layer, rows in sizes.items():
                u[s, layer, span - rows:span] = jnp.zeros((rows, ch), BF16)

    @pl.when(me < far_hops)
    def _():
        for s in range(batch):
            u[s, last, :span] = jnp.zeros((span, ch), BF16)

    @pl.when(me < chip)
    def _():
        pl.semaphore_wait(barrier, 1)
        greet_other_chip()

    @pl.when(me >= chip)
    def _():
        pl.semaphore_wait(barrier, n_sp - 1)
        greet_other_chip()

    for layer in range(1, AHEAD):
        start_weights(layer)
    sig_in.wait()
    cond_in.wait()

    def send_first():
        for s in range(batch):
            edge_copy(s, 0, sizes[0]).start()
            cond_copy(s).start()

    @pl.when(me == chip - 1)
    def _():
        pl.semaphore_wait(barrier, chip)

    @pl.when(me + 1 < n_sp)
    def _():
        send_first()

    for s in range(batch):
        h[s, TILE:] = u[s, 0, span:].astype(F32)
        h[s, :TILE] = jnp.zeros((TILE, ch), F32)
    bias_in.wait()

    def gate(z):
        half = ch // 2
        parts = []
        for lo in (0, half):
            zf, zg = z(lo, lo + half), z(ch + lo, ch + lo + half)
            parts.append((jnp.tanh(zf) * (0.5 * jnp.tanh(0.5 * zg) + 0.5)).astype(BF16))
        return jnp.concatenate(parts, axis=1)

    def step(s, layer):
        @pl.when(s == 0)
        def _():
            @pl.when(layer < layers - AHEAD)
            def _():
                start_weights(layer + AHEAD)

            await_weights(layer)

        dilation = jnp.left_shift(1, layer)

        def layer_body(ahead, past):
            x = jnp.concatenate([u[s, layer, span - ahead:], c[s, TILE - ahead:], past], axis=1)
            a = gate(lambda lo, hi: jnp.dot(x, w_in[layer, :, lo:hi], preferred_element_type=F32) + bias[pl.ds(layer, 1), lo:hi])
            acts[s, layer] = a[ahead:]
            new_h = h[s, TILE - ahead:] + jnp.dot(a, w_mix[layer], preferred_element_type=F32)
            h[s, TILE - ahead:] = new_h
            new_u = new_h.astype(BF16)
            u[s, layer + 1, span:] = new_u[ahead:]
            return new_u[:ahead]

        def small():
            @pl.when((layer == 0) & (me >= 1))
            def _():
                edge_copy(s, 0, sizes[0]).wait_recv()
                cond_copy(s).wait_recv()
                h[s, :TILE] = u[s, 0, span - TILE:span].astype(F32)

            wide = u[s, layer, span - 2 * TILE:].astype(F32)
            edge = layer_body(TILE, pltpu.roll(wide, dilation, axis=0)[TILE:].astype(BF16))

            def keep_edge():
                u[s, layer + 1, span - TILE:span] = jnp.where(me > 0, edge, jnp.zeros_like(edge))

            def send():
                @pl.when(me + 1 < n_sp)
                def _():
                    edge_copy(s, near, sizes[near]).start()

            lax.cond(layer + 1 < near, keep_edge, send)

            @pl.when((layer == 0) & (s == 0) & (me < chip - 1))
            def _():
                pl.semaphore_wait(barrier, chip)

        def large():
            @pl.when((s == 1) & (layer == near))
            def _():
                for k in range(layers):
                    pltpu.make_async_copy(w_skip.at[k], w_sum.at[k], sum_sem).start()

            @pl.when(me >= 1)
            def _():
                pick(layer, exchanged, lambda k: edge_copy(s, k, sizes[k]).wait_recv())

            base = pl.multiple_of(span - jnp.minimum(dilation, span), TILE)
            layer_body(0, u[s, layer, pl.ds(base, span)])

            @pl.when((me + 1 < n_sp) & (layer + 1 < last))
            def _():
                pick(layer + 1, exchanged[1:], lambda k: edge_copy(s, k, sizes[k]).start())

        lax.cond(layer < near, small, large)

        @pl.when(sends_far)
        def _():
            def pieces(s, first, end):
                for piece in range(first, end):
                    far_copy(s, piece).start()

            def first_sequence():
                @pl.when(layer == last - 1)
                def _():
                    pieces(0, 0, 1)

            def second_sequence():
                pick(layer, list(range(last)), lambda k: (
                    pieces(0, 1, 3) if k == 0 else pieces(0, k + 2, k + 3) if k < 6
                    else pieces(1, 0, PIECES) if k == last - 1 else None))

            lax.cond(s == 0, first_sequence, second_sequence)

    def last_step(s):
        @pl.when(s == 0)
        def _():
            await_weights(last)

        x = jnp.concatenate([u[s, last, span:], c[s, TILE:]], axis=1)
        depth = x.shape[1]
        z_part[...] = jnp.dot(x, w_in[last, :depth], preferred_element_type=F32) + bias[last:, :]

        rows = span // 2

        def finish(part, carry):
            at = pl.ds(pl.multiple_of(part * rows, rows), rows)

            @pl.when(me >= far_hops)
            def _():
                landed(u.at[s, last, at], far_recv_sem.at[s, part])

            past = u[s, last, at]
            a = gate(lambda lo, hi: z_part[at, lo:hi] + jnp.dot(past, w_in[last, depth:, lo:hi], preferred_element_type=F32))
            h_out[s, at] = h[s, pl.ds(pl.multiple_of(TILE + part * rows, TILE), rows)] + jnp.dot(a, w_mix[last], preferred_element_type=F32)
            x = jnp.concatenate([acts[s, last - 1, at], a], axis=1)
            skip[s, at] += jnp.dot(x, w_sum[last - 1:].reshape(2 * ch, skip.shape[2]), preferred_element_type=F32)
            return carry

        lax.fori_loop(0, 2, finish, 0, unroll=True)

    def sum_skip(s):
        @pl.when(s == 0)
        def _():
            landed(w_sum, sum_sem)

        x = jnp.concatenate([acts[s, k] for k in range(last - 1)], axis=1)
        skip[s] = jnp.dot(x, w_sum[:last - 1].reshape((last - 1) * ch, skip.shape[2]), preferred_element_type=F32)

    early = [2 * k for k in range(9)] + [2 * k + 1 for k in range(9)] + [20, 21, 18, 19]
    late = [0, 2, 4, 6, 1, 3, 5, 7] + [2 * k for k in range(4, 9)] + [2 * k + 1 for k in range(4, 8)] + [20, 18, 21, 17, 19]

    def run(i, carry):
        code = jnp.where(me < n_sp // 2, at_step(i, early), at_step(i, late))
        s, layer = lax.rem(code, batch), lax.div(code, batch)

        lax.cond(layer < last, lambda: step(s, layer),
                 lambda: lax.cond(layer == last, lambda: last_step(s), lambda: sum_skip(s)))
        return carry

    lax.fori_loop(0, len(early), run, 0)

    total = sum(sizes.values())
    parts = next(n for n in range(1, layers) if total % (n * TILE) == 0 and total <= n * 2 * span)
    for s in range(batch):
        @pl.when(me + 1 < n_sp)
        def _():
            landed(u.at[s, pl.ds(0, parts), pl.ds(0, total // parts)], send_sem.at[s])

        @pl.when(sends_far)
        def _():
            landed(u.at[s, last, pl.ds(0, span)], far_send_sem.at[s])

    @pl.when(me + 1 < n_sp)
    def _():
        landed(c.at[:, pl.ds(span, TILE)], cond_send_sem)


def store_kernel(h, skip, h_out, skip_out, sem):
    copies = [pltpu.make_async_copy(h, h_out, sem.at[0]), pltpu.make_async_copy(skip, skip_out, sem.at[1])]
    for copy in copies:
        copy.start()
    for copy in copies:
        copy.wait()


def solution(mesh):
    n_sp = mesh.shape['sp']

    def local_stack(signal, cond_feats, w_now, w_past, w_cond, b_gate, w_res, w_skip):
        batch, span, ch = signal.shape
        layers, cond_ch, skip_ch = w_now.shape[0], cond_feats.shape[2], w_skip.shape[2]
        in_vmem = pl.BlockSpec(memory_space=pltpu.VMEM)
        h, skip = pl.pallas_call(
            functools.partial(stack_kernel, n_sp),
            out_shape=[pltpu.VMEM((batch, span, ch), F32), pltpu.VMEM((batch, span, skip_ch), F32)],
            in_specs=[pl.BlockSpec(memory_space=pltpu.HBM)] * 8,
            out_specs=[in_vmem] * 2,
            scratch_shapes=[
                pltpu.VMEM((batch, layers, 2 * span, ch), BF16),
                pltpu.VMEM((batch, span + TILE, ch), F32),
                pltpu.VMEM((batch, layers - 1, span, ch), BF16),
                pltpu.VMEM((span, 2 * ch), F32),
                pltpu.VMEM((batch, span + TILE, cond_ch), BF16),
                pltpu.VMEM((layers, 2 * ch), F32),
                pltpu.VMEM((layers, 2 * ch + cond_ch, 2 * ch), BF16),
                pltpu.VMEM((layers, ch, ch), BF16),
                pltpu.VMEM((layers, ch, skip_ch), BF16),
                pltpu.SemaphoreType.DMA,
                pltpu.SemaphoreType.DMA,
                pltpu.SemaphoreType.DMA,
                pltpu.SemaphoreType.DMA((AHEAD + 1, 2)),
                pltpu.SemaphoreType.DMA,
                pltpu.SemaphoreType.DMA((batch,)),
                pltpu.SemaphoreType.DMA((batch, 6)),
                pltpu.SemaphoreType.DMA((batch,)),
                pltpu.SemaphoreType.DMA((batch, 2)),
                pltpu.SemaphoreType.DMA,
                pltpu.SemaphoreType.DMA((batch,)),
            ],
            compiler_params=pltpu.CompilerParams(collective_id=0, has_side_effects=True, vmem_limit_bytes=60 * 2 ** 20),
        )(signal, cond_feats, w_now, w_past, w_cond, b_gate, w_res, w_skip)
        return pl.pallas_call(
            store_kernel,
            out_shape=[jax.ShapeDtypeStruct((batch, span, ch), F32), jax.ShapeDtypeStruct((batch, span, skip_ch), F32)],
            in_specs=[in_vmem] * 2,
            out_specs=[pl.BlockSpec(memory_space=pl.ANY)] * 2,
            scratch_shapes=[pltpu.SemaphoreType.DMA((2,))],
            compiler_params=pltpu.CompilerParams(vmem_limit_bytes=2 ** 20),
        )(h, skip)

    seq_spec = P('dp', 'sp', None)
    return jax.shard_map(local_stack, mesh=mesh,
                         in_specs=(seq_spec, seq_spec, P(), P(), P(), P(), P(), P()),
                         out_specs=(seq_spec, seq_spec), check_vma=False)
```

```python
import functools

import jax
import jax.numpy as jnp
from jax import lax
from jax.experimental import pallas as pl
from jax.experimental.pallas import tpu as pltpu
from jax.sharding import PartitionSpec as P

BF16, F32 = jnp.bfloat16, jnp.float32
MESH = pl.DeviceIdType.MESH
TILE = 16
AHEAD = 2
PIECES = 8


def at_step(i, order):
    code = 2 * i + (order[-1] - 2 * (len(order) - 1))
    for j in range(len(order) - 2, -1, -1):
        if order[j] - 2 * j != order[j + 1] - 2 * (j + 1):
            code = jnp.where(i <= j, 2 * i + (order[j] - 2 * j), code)
    return code


def stack_kernel(n_sp, signal, cond, w_now, w_past, w_cond, b_gate, w_res, w_skip, h_out, skip,
                 u, h, acts, z_part, c, bias, w_in, w_mix, w_sum,
                 sig_sem, cond_sem, bias_sem, w_sem, sum_sem, send_sem, recv_sem, far_send_sem, far_recv_sem,
                 cond_send_sem, cond_recv_sem):
    batch, layers, span, ch = u.shape[0], w_in.shape[0], h_out.shape[1], h_out.shape[2]
    last, cond_ch = layers - 1, c.shape[2]
    dp, me = lax.axis_index('dp'), lax.axis_index('sp')

    near = next(k for k in range(layers) if 2 ** k >= TILE)
    sizes = {k: min(max(TILE, 2 ** k), span) for k in range(last) if k == 0 or k >= near}
    far_hops = 2 ** last // span

    def start_weights(layer):
        slot = lax.rem(layer, AHEAD + 1)
        for src, dst in ((w_now.at[layer], w_in.at[layer, pl.ds(0, ch)]),
                         (w_cond.at[layer], w_in.at[layer, pl.ds(ch, cond_ch)]),
                         (w_past.at[layer], w_in.at[layer, pl.ds(ch + cond_ch, ch)])):
            pltpu.make_async_copy(src, dst, w_sem.at[slot, 0]).start()
        pltpu.make_async_copy(w_res.at[layer], w_mix.at[layer], w_sem.at[slot, 1]).start()

    def landed(ref, sem):
        pltpu.make_async_copy(ref, ref, sem).wait()

    def await_weights(layer):
        slot = lax.rem(layer, AHEAD + 1)
        landed(w_in.at[layer], w_sem.at[slot, 0])
        landed(w_mix.at[layer], w_sem.at[slot, 1])

    def edge_copy(s, layer, rows):
        return pltpu.make_async_remote_copy(
            src_ref=u.at[s, layer, pl.ds(2 * span - rows, rows)],
            dst_ref=u.at[s, layer, pl.ds(span - rows, rows)],
            send_sem=send_sem.at[s], recv_sem=recv_sem.at[s, layer if layer < 1 else layer - near + 1],
            device_id=(dp, lax.rem(me + 1, n_sp)), device_id_type=MESH)

    def pick(layer, layers, act):
        if len(layers) == 1:
            act(layers[0])
            return
        middle = len(layers) // 2
        lax.cond(layer < layers[middle],
                 lambda: pick(layer, layers[:middle], act), lambda: pick(layer, layers[middle:], act))

    exchanged = list(range(near, last))

    def cond_copy(s):
        return pltpu.make_async_remote_copy(
            src_ref=c.at[s, pl.ds(span, TILE)], dst_ref=c.at[s, pl.ds(0, TILE)],
            send_sem=cond_send_sem, recv_sem=cond_recv_sem.at[s],
            device_id=(dp, lax.rem(me + 1, n_sp)), device_id_type=MESH)

    def far_copy(s, piece):
        rows = span // PIECES
        return pltpu.make_async_remote_copy(
            src_ref=u.at[s, last, pl.ds(span + piece * rows, rows)],
            dst_ref=u.at[s, last, pl.ds(piece * rows, rows)],
            send_sem=far_send_sem.at[s], recv_sem=far_recv_sem.at[s, piece // (PIECES // 2)],
            device_id=(dp, lax.rem(me + far_hops, n_sp)), device_id_type=MESH)

    sends_far = me + far_hops < n_sp

    sig_in = pltpu.make_async_copy(signal, u.at[:, 0, pl.ds(span, span)], sig_sem)
    cond_in = pltpu.make_async_copy(cond, c.at[:, pl.ds(TILE, span)], cond_sem)
    bias_in = pltpu.make_async_copy(b_gate, bias, bias_sem)
    for copy in (sig_in, cond_in, bias_in):
        copy.start()
    start_weights(0)

    barrier = pltpu.get_barrier_semaphore()
    chip = n_sp // 2
    partner = me + 1 - 2 * lax.rem(me, 2)
    pl.semaphore_signal(barrier, inc=1, device_id=(dp, partner), device_id_type=MESH)

    def greet_other_chip():
        for core in range(chip):
            pl.semaphore_signal(barrier, inc=1, device_id=(dp, (1 - me // chip) * chip + core), device_id_type=MESH)

    @pl.when(me < 1)
    def _():
        for s in range(batch):
            for layer, rows in sizes.items():
                u[s, layer, span - rows:span] = jnp.zeros((rows, ch), BF16)

    @pl.when(me < far_hops)
    def _():
        for s in range(batch):
            u[s, last, :span] = jnp.zeros((span, ch), BF16)

    @pl.when(me < chip)
    def _():
        pl.semaphore_wait(barrier, 1)
        greet_other_chip()

    @pl.when(me >= chip)
    def _():
        pl.semaphore_wait(barrier, n_sp - 1)
        greet_other_chip()

    for layer in range(1, AHEAD):
        start_weights(layer)
    sig_in.wait()
    cond_in.wait()

    def send_first():
        for s in range(batch):
            edge_copy(s, 0, sizes[0]).start()
            cond_copy(s).start()

    @pl.when(me == chip - 1)
    def _():
        pl.semaphore_wait(barrier, chip)

    @pl.when(me + 1 < n_sp)
    def _():
        send_first()

    for s in range(batch):
        h[s, TILE:] = u[s, 0, span:].astype(F32)
        h[s, :TILE] = jnp.zeros((TILE, ch), F32)
    bias_in.wait()

    def gate(z):
        half = ch // 2
        parts = []
        for lo in (0, half):
            zf, zg = z(lo, lo + half), z(ch + lo, ch + lo + half)
            parts.append((jnp.tanh(zf) * (0.5 * jnp.tanh(0.5 * zg) + 0.5)).astype(BF16))
        return jnp.concatenate(parts, axis=1)

    def step(s, layer):
        @pl.when(s == 0)
        def _():
            @pl.when(layer < layers - AHEAD)
            def _():
                start_weights(layer + AHEAD)

            await_weights(layer)

        dilation = jnp.left_shift(1, layer)

        def layer_body(ahead, past):
            x = jnp.concatenate([u[s, layer, span - ahead:], c[s, TILE - ahead:], past], axis=1)
            a = gate(lambda lo, hi: jnp.dot(x, w_in[layer, :, lo:hi], preferred_element_type=F32) + bias[pl.ds(layer, 1), lo:hi])
            acts[s, layer] = a[ahead:]
            new_h = h[s, TILE - ahead:] + jnp.dot(a, w_mix[layer], preferred_element_type=F32)
            h[s, TILE - ahead:] = new_h
            new_u = new_h.astype(BF16)
            u[s, layer + 1, span:] = new_u[ahead:]
            return new_u[:ahead]

        def small():
            @pl.when((layer == 0) & (me >= 1))
            def _():
                edge_copy(s, 0, sizes[0]).wait_recv()
                cond_copy(s).wait_recv()
                h[s, :TILE] = u[s, 0, span - TILE:span].astype(F32)

            wide = u[s, layer, span - 2 * TILE:].astype(F32)
            edge = layer_body(TILE, pltpu.roll(wide, dilation, axis=0)[TILE:].astype(BF16))

            def keep_edge():
                u[s, layer + 1, span - TILE:span] = jnp.where(me > 0, edge, jnp.zeros_like(edge))

            def send():
                @pl.when(me + 1 < n_sp)
                def _():
                    edge_copy(s, near, sizes[near]).start()

            lax.cond(layer + 1 < near, keep_edge, send)

            @pl.when((layer == 0) & (s == 0) & (me < chip - 1))
            def _():
                pl.semaphore_wait(barrier, chip)

        def large():
            @pl.when((s == 1) & (layer == near))
            def _():
                for k in range(layers):
                    pltpu.make_async_copy(w_skip.at[k], w_sum.at[k], sum_sem).start()

            @pl.when(me >= 1)
            def _():
                pick(layer, exchanged, lambda k: edge_copy(s, k, sizes[k]).wait_recv())

            base = pl.multiple_of(span - jnp.minimum(dilation, span), TILE)
            layer_body(0, u[s, layer, pl.ds(base, span)])

            @pl.when((me + 1 < n_sp) & (layer + 1 < last))
            def _():
                pick(layer + 1, exchanged[1:], lambda k: edge_copy(s, k, sizes[k]).start())

        lax.cond(layer < near, small, large)

        @pl.when(sends_far)
        def _():
            def pieces(s, first, end):
                for piece in range(first, end):
                    far_copy(s, piece).start()

            def first_sequence():
                @pl.when(layer == last - 1)
                def _():
                    pieces(0, 0, 1)

            def second_sequence():
                pick(layer, list(range(last)), lambda k: (
                    pieces(0, 1, 3) if k == 0 else pieces(0, k + 2, k + 3) if k < 6
                    else pieces(1, 0, PIECES) if k == last - 1 else None))

            lax.cond(s == 0, first_sequence, second_sequence)

    def last_step(s):
        @pl.when(s == 0)
        def _():
            await_weights(last)

        x = jnp.concatenate([u[s, last, span:], c[s, TILE:]], axis=1)
        depth = x.shape[1]
        z_part[...] = jnp.dot(x, w_in[last, :depth], preferred_element_type=F32) + bias[last:, :]

        skip[s] += jnp.dot(acts[s, last - 1], w_sum[last - 1], preferred_element_type=F32)

        rows = span // 2

        def finish(part, carry):
            at = pl.ds(pl.multiple_of(part * rows, rows), rows)

            @pl.when(me >= far_hops)
            def _():
                landed(u.at[s, last, at], far_recv_sem.at[s, part])

            past = u[s, last, at]
            a = gate(lambda lo, hi: z_part[at, lo:hi] + jnp.dot(past, w_in[last, depth:, lo:hi], preferred_element_type=F32))
            h_out[s, at] = h[s, pl.ds(pl.multiple_of(TILE + part * rows, TILE), rows)] + jnp.dot(a, w_mix[last], preferred_element_type=F32)
            skip[s, at] += jnp.dot(a, w_sum[last], preferred_element_type=F32)
            return carry

        lax.fori_loop(0, 2, finish, 0, unroll=True)

    def sum_skip(s):
        @pl.when(s == 0)
        def _():
            landed(w_sum, sum_sem)

        x = jnp.concatenate([acts[s, k] for k in range(last - 1)], axis=1)
        skip[s] = jnp.dot(x, w_sum[:last - 1].reshape((last - 1) * ch, skip.shape[2]), preferred_element_type=F32)

    early = [2 * k for k in range(9)] + [2 * k + 1 for k in range(9)] + [20, 21, 18, 19]
    late = [0, 2, 4, 6, 1, 3, 5, 7] + [2 * k for k in range(4, 9)] + [2 * k + 1 for k in range(4, 8)] + [20, 18, 21, 17, 19]

    def run(i, carry):
        code = jnp.where(me < n_sp // 2, at_step(i, early), at_step(i, late))
        s, layer = lax.rem(code, batch), lax.div(code, batch)

        lax.cond(layer < last, lambda: step(s, layer),
                 lambda: lax.cond(layer == last, lambda: last_step(s), lambda: sum_skip(s)))
        return carry

    lax.fori_loop(0, len(early), run, 0)

    total = sum(sizes.values())
    parts = next(n for n in range(1, layers) if total % (n * TILE) == 0 and total <= n * 2 * span)
    for s in range(batch):
        @pl.when(me + 1 < n_sp)
        def _():
            landed(u.at[s, pl.ds(0, parts), pl.ds(0, total // parts)], send_sem.at[s])

        @pl.when(sends_far)
        def _():
            landed(u.at[s, last, pl.ds(0, span)], far_send_sem.at[s])

    @pl.when(me + 1 < n_sp)
    def _():
        landed(c.at[:, pl.ds(span, TILE)], cond_send_sem)


def store_kernel(h, skip, h_out, skip_out, sem):
    copies = [pltpu.make_async_copy(h, h_out, sem.at[0]), pltpu.make_async_copy(skip, skip_out, sem.at[1])]
    for copy in copies:
        copy.start()
    for copy in copies:
        copy.wait()


def solution(mesh):
    n_sp = mesh.shape['sp']

    def local_stack(signal, cond_feats, w_now, w_past, w_cond, b_gate, w_res, w_skip):
        batch, span, ch = signal.shape
        layers, cond_ch, skip_ch = w_now.shape[0], cond_feats.shape[2], w_skip.shape[2]
        in_vmem = pl.BlockSpec(memory_space=pltpu.VMEM)
        h, skip = pl.pallas_call(
            functools.partial(stack_kernel, n_sp),
            out_shape=[pltpu.VMEM((batch, span, ch), F32), pltpu.VMEM((batch, span, skip_ch), F32)],
            in_specs=[pl.BlockSpec(memory_space=pltpu.HBM)] * 8,
            out_specs=[in_vmem] * 2,
            scratch_shapes=[
                pltpu.VMEM((batch, layers, 2 * span, ch), BF16),
                pltpu.VMEM((batch, span + TILE, ch), F32),
                pltpu.VMEM((batch, layers - 1, span, ch), BF16),
                pltpu.VMEM((span, 2 * ch), F32),
                pltpu.VMEM((batch, span + TILE, cond_ch), BF16),
                pltpu.VMEM((layers, 2 * ch), F32),
                pltpu.VMEM((layers, 2 * ch + cond_ch, 2 * ch), BF16),
                pltpu.VMEM((layers, ch, ch), BF16),
                pltpu.VMEM((layers, ch, skip_ch), BF16),
                pltpu.SemaphoreType.DMA,
                pltpu.SemaphoreType.DMA,
                pltpu.SemaphoreType.DMA,
                pltpu.SemaphoreType.DMA((AHEAD + 1, 2)),
                pltpu.SemaphoreType.DMA,
                pltpu.SemaphoreType.DMA((batch,)),
                pltpu.SemaphoreType.DMA((batch, 6)),
                pltpu.SemaphoreType.DMA((batch,)),
                pltpu.SemaphoreType.DMA((batch, 2)),
                pltpu.SemaphoreType.DMA,
                pltpu.SemaphoreType.DMA((batch,)),
            ],
            compiler_params=pltpu.CompilerParams(collective_id=0, has_side_effects=True, vmem_limit_bytes=60 * 2 ** 20),
        )(signal, cond_feats, w_now, w_past, w_cond, b_gate, w_res, w_skip)
        return pl.pallas_call(
            store_kernel,
            out_shape=[jax.ShapeDtypeStruct((batch, span, ch), F32), jax.ShapeDtypeStruct((batch, span, skip_ch), F32)],
            in_specs=[in_vmem] * 2,
            out_specs=[pl.BlockSpec(memory_space=pl.ANY)] * 2,
            scratch_shapes=[pltpu.SemaphoreType.DMA((2,))],
            compiler_params=pltpu.CompilerParams(vmem_limit_bytes=2 ** 20),
        )(h, skip)

    seq_spec = P('dp', 'sp', None)
    return jax.shard_map(local_stack, mesh=mesh,
                         in_specs=(seq_spec, seq_spec, P(), P(), P(), P(), P(), P()),
                         out_specs=(seq_spec, seq_spec), check_vma=False)
```
